512 devices in a mesh: member: 8 (over y_hi, x), space: 64 (over z, y_lo, core).
Axes of the slice: x: 4, y: 8 (y_hi: 2, y_lo: 4; y = y_hi * 4 + y_lo), z: 8, core: 2. Of those that a mesh axis runs over, the one named last changes fastest.
Arguments:
- node_states: bfloat16 [16384, 1024], P('space'), may hold values from -6 to 6
- noise: bfloat16 [8, 16, 16384], P('member', None, 'space'), may hold values from -4 to 4
- norm_gain: float32 [1024], replicated, may hold values from 0.5 to 1.5
- cond_weight: bfloat16 [16, 2048], replicated, may hold values from -1.5 to 1.5
- w_query: bfloat16 [1024, 1024], P('space'), may hold values from -0.1875 to 0.1875
- w_key: bfloat16 [1024, 1024], P('space'), may hold values from -0.1875 to 0.1875
- w_value: bfloat16 [1024, 1024], P('space'), may hold values from -0.1875 to 0.1875
- w_out: bfloat16 [1024, 1024], P('space'), may hold values from -0.1875 to 0.1875
- edge_src: int32 [8, 16384], P(None, 'space'), may hold values from 0 to 511, as said below
- send_rows: int32 [16384], P('space'), may hold values from 0 to 255, as said below
- dec_src: int32 [3, 65536], P(None, 'space'), may hold values from 0 to 255
- dec_weight: float32 [3, 65536], P(None, 'space'), may hold values from 0.2 to 1
- w_decode: bfloat16 [100, 1024], replicated, may hold values from -0.1875 to 0.1875
- truth: bfloat16 [100, 65536], P(None, 'space'), may hold values from -6 to 6
- area: float32 [65536], P('space'), may hold values from 0.1 to 3.5
Outputs:
- loss: float32 [], replicated
- field_grad: bfloat16 [8, 100, 65536], P('member', None, 'space')
The draws below stay inside these ranges and needn't reach their ends.
Inputs may be any that keep to these rules, and one draw needn't show every extreme that they name: `send_rows`: each block's 2 * 128 entries are distinct node indices within that block. `edge_src`: entries below 128 name a row of the previous block's halo rows, entries from 384 on a row of the next block's; of each such halo half only a leading part of at least 64 rows is named, its length varying by block, and in some block the whole half is named.
All inputs are finite; a program needn't handle non-finite values.
Results may differ from the reference program's by a relative error of at most 0.015.
Values may be sent and summed in bfloat16 or wider, within the bound.
A program may use at most 64 MiB of HBM per device.

```python
import math
import jax
import jax.numpy as jnp
from jax import lax

H = 1024
HEADS = 16
NOISE = 16
VARS = 100
KNB = 8
DEC_K = 3
HALO = 128
NODE_DEV = 256
GRID_DEV = 1024
MEMBERS = 8
NODES = 16384
GRID = 65536


def live_counts(key):
    devices = NODES // NODE_DEV
    counts = jax.random.randint(jax.random.fold_in(key, 7), (2, devices), HALO // 2, HALO + 1)
    return counts.at[:, 0].set(HALO).astype(jnp.int32)


def draw_send_rows(key, part):
    devices = NODES // NODE_DEV
    subkeys = jax.random.split(jax.random.fold_in(key, 11), devices)

    def choose(subkey):
        return jax.random.permutation(subkey, NODE_DEV)[:2 * HALO]
    chosen = jax.vmap(choose)(subkeys)
    return chosen.reshape(-1).astype(jnp.int32)


def draw_edge_src(key, part):
    devices = NODES // NODE_DEV
    counts = live_counts(key)
    anchor = jax.random.fold_in(key, 13)
    shape = (KNB, devices, NODE_DEV)
    region = jax.random.randint(jax.random.fold_in(anchor, 1), shape, 0, 8)
    local_pick = jax.random.randint(jax.random.fold_in(anchor, 2), shape, 0, NODE_DEV)
    left_pick = jax.random.randint(jax.random.fold_in(anchor, 3), shape, 0, counts[0][None, :, None])
    right_pick = jax.random.randint(jax.random.fold_in(anchor, 4), shape, 0, counts[1][None, :, None])
    chosen = jnp.where(region < 6, HALO + local_pick, jnp.where(region == 6, left_pick, HALO + NODE_DEV + right_pick))
    return chosen.reshape(KNB, NODES).astype(jnp.int32)


def draw_area(key, part):
    position = (jnp.arange(GRID, dtype=jnp.int32) % GRID_DEV).astype(jnp.float32) / GRID_DEV
    anchor = jax.random.fold_in(key, 17)
    rough = jnp.exp(jax.random.uniform(anchor, (GRID,), jnp.float32, jnp.log(0.5), 0.0))
    return (0.25 * jnp.exp(position * jnp.log(8.0)) * rough).astype(jnp.float32)


def with_ends(array, stream_key, low, largest):
    index_at = [jax.random.randint(jax.random.fold_in(stream_key, axis), (), 0, length) for axis, length in enumerate(array.shape)]
    widest = array.shape.index(max(array.shape))
    beside = index_at[:widest] + [(index_at[widest] + 1) % array.shape[widest]] + index_at[widest + 1:]
    return array.at[tuple(index_at)].set(low).at[tuple(beside)].set(largest)


def level_of(key, shape, shards, low, largest):
    gain = 1.0
    for dim, parts in shards:
        heights = jax.random.uniform(jax.random.fold_in(jax.random.fold_in(key, 6), dim), (parts,), jnp.float32, low / len(shards), largest / len(shards))
        gain = gain * jnp.repeat(jnp.exp(heights), shape[dim] // parts).reshape((-1,) + (1,) * (len(shape) - 1 - dim))
    return gain


def centred(stream_key, shape, scale, reach, shards=(), kind=jnp.bfloat16):
    drawn = scale * jax.random.normal(stream_key, shape, jnp.float32)
    if shards:
        drawn = drawn * level_of(stream_key, shape, shards, -0.22, 0.18)
    return jnp.clip(drawn, -reach, reach).astype(kind)


def setup_inputs(seed: int = 0) -> dict:
    seeds = jax.random.split(jax.random.key(seed), 16)
    node_states = centred(seeds[0], (NODES, H), 1.0, 6.0, ((0, 64),))
    noise = centred(seeds[1], (MEMBERS, NOISE, NODES), 0.5, 4.0, ((0, 8), (2, 64)))
    norm_gain = jnp.clip(1.0 + 0.1 * jax.random.normal(seeds[2], (H,), jnp.float32), 0.5, 1.5)
    cond_weight = centred(seeds[3], (NOISE, 2 * H), NOISE ** -0.5, 1.5)
    w_query = centred(seeds[4], (H, H), H ** -0.5, 0.1875, ((0, 64),))
    w_key = centred(seeds[5], (H, H), H ** -0.5, 0.1875, ((0, 64),))
    w_value = centred(seeds[6], (H, H), H ** -0.5, 0.1875, ((0, 64),))
    w_out = centred(seeds[7], (H, H), H ** -0.5, 0.1875, ((0, 64),))
    edge_src = draw_edge_src(jax.random.fold_in(seeds[15], 71), 0)
    send_rows = draw_send_rows(jax.random.fold_in(seeds[15], 71), 0)
    dec_src = with_ends(jax.random.randint(seeds[10], (DEC_K, GRID), 0, NODE_DEV), jax.random.fold_in(seeds[10], 1), 0, NODE_DEV - 1).astype(jnp.int32)
    dec_weight = jnp.clip(jnp.exp(math.log(1.0) - 1.609438 * jax.random.uniform(seeds[11], (DEC_K, GRID), jnp.float32) ** level_of(seeds[11], (DEC_K, GRID), ((1, 64),), -0.2, 0.2)), 0.2, 1.0)
    w_decode = centred(seeds[12], (VARS, H), H ** -0.5, 0.1875)
    truth = centred(seeds[13], (VARS, GRID), 1.0, 6.0, ((1, 64),))
    area = draw_area(jax.random.fold_in(seeds[15], 71), 0)
    return dict(node_states=node_states, noise=noise, norm_gain=norm_gain, cond_weight=cond_weight, w_query=w_query, w_key=w_key, w_value=w_value, w_out=w_out, edge_src=edge_src, send_rows=send_rows, dec_src=dec_src, dec_weight=dec_weight, w_decode=w_decode, truth=truth, area=area)


SMOOTH = 0.25
EPS = 1e-05

def condition(states, noise_block, norm_gain, cond_weight):
    values = states.astype(jnp.float32)
    center = values - lax.optimization_barrier(jnp.mean(values, axis=1, keepdims=True))
    spread = lax.optimization_barrier(jnp.mean(center * center, axis=1, keepdims=True))
    normed = center * lax.rsqrt(spread + EPS)
    terms = lax.dot_general(noise_block, cond_weight, (((0,), (0,)), ((), ())), preferred_element_type=jnp.float32)
    model_width = states.shape[1]
    return (normed * norm_gain * (1.0 + terms[:, :model_width]) + terms[:, model_width:]).astype(jnp.bfloat16)

def attention(query_rows, key_ext, value_ext, sources):
    row_count, model_width = query_rows.shape
    head_size = model_width // HEADS
    factor = 1.0 / head_size ** 0.5
    query_wide = query_rows.astype(jnp.float32).reshape(row_count, HEADS, head_size)
    numerator = jnp.zeros((row_count, HEADS, head_size), jnp.float32)
    denominator = jnp.zeros((row_count, HEADS), jnp.float32)
    for slot_index in range(sources.shape[0]):
        picked = sources[slot_index]
        gathered_key = key_ext[picked].astype(jnp.float32).reshape(row_count, HEADS, head_size)
        weight = jnp.exp(lax.optimization_barrier(jnp.sum(query_wide * gathered_key, axis=2)) * factor)
        gathered_value = value_ext[picked].astype(jnp.float32).reshape(row_count, HEADS, head_size)
        numerator = numerator + weight[:, :, None] * gathered_value
        denominator = denominator + weight
    return (numerator / denominator[:, :, None]).reshape(row_count, model_width).astype(jnp.bfloat16)

def decode(processed, sources, dec_weight, w_decode):
    gathered = jnp.zeros((sources.shape[1], processed.shape[1]), jnp.float32)
    for neighbour in range(sources.shape[0]):
        gathered = gathered + dec_weight[neighbour][:, None] * processed[sources[neighbour]].astype(jnp.float32)
    return lax.dot_general(w_decode, gathered.astype(jnp.bfloat16), (((1,), (1,)), ((), ())), preferred_element_type=jnp.float32).astype(jnp.bfloat16)

def smooth_abs(difference):
    return jnp.sqrt(difference * difference + SMOOTH * SMOOTH)

def reference(node_states, noise, norm_gain, cond_weight, w_query, w_key, w_value, w_out, edge_src, send_rows, dec_src, dec_weight, w_decode, truth, area):
    devices = NODES // NODE_DEV
    send_table = send_rows.reshape(devices, 2 * HALO).astype(jnp.int32)
    node_base = (jnp.arange(devices, dtype=jnp.int32) * NODE_DEV).astype(jnp.int32)
    left_block = jnp.roll(send_table[:, HALO:] + node_base[:, None], 1, axis=0)
    right_block = jnp.roll(send_table[:, :HALO] + node_base[:, None], -1, axis=0)
    own_block = node_base[:, None] + jnp.arange(NODE_DEV, dtype=jnp.int32)[None, :]
    extended = jnp.concatenate((left_block, own_block, right_block), axis=1).astype(jnp.int32)
    local_edges = edge_src.reshape(KNB, devices, NODE_DEV).astype(jnp.int32)
    broad = jnp.broadcast_to(extended[None], (KNB, devices, NODE_DEV + 2 * HALO))
    global_edges = jnp.take_along_axis(broad, local_edges, axis=2).reshape(KNB, NODES).astype(jnp.int32)
    global_dec = (dec_src.reshape(DEC_K, devices, GRID_DEV) + node_base[None, :, None]).reshape(DEC_K, GRID).astype(jnp.int32)
    field_list = []
    for member_index in range(MEMBERS):
        hidden = condition(node_states, noise[member_index], norm_gain, cond_weight)
        query_rows = jnp.dot(hidden, w_query, preferred_element_type=jnp.float32).astype(jnp.bfloat16)
        key_rows = jnp.dot(hidden, w_key, preferred_element_type=jnp.float32).astype(jnp.bfloat16)
        value_rows = jnp.dot(hidden, w_value, preferred_element_type=jnp.float32).astype(jnp.bfloat16)
        attended = attention(query_rows, key_rows, value_rows, global_edges)
        update = jnp.dot(attended, w_out, preferred_element_type=jnp.float32)
        processed = (node_states.astype(jnp.float32) + update).astype(jnp.bfloat16)
        field_list.append(decode(processed, global_dec, dec_weight, w_decode))
    values = jnp.stack(field_list).astype(jnp.float32)
    members = MEMBERS
    truth_wide = truth.astype(jnp.float32)
    skill_gap = values - truth_wide[None]
    skill_abs = smooth_abs(skill_gap)
    spread_abs = jnp.zeros_like(values)
    spread_slope = jnp.zeros_like(values)
    for other_member in range(members):
        difference = values - values[other_member][None]
        magnitude = smooth_abs(difference)
        spread_abs = spread_abs + magnitude
        spread_slope = spread_slope + difference / magnitude
    pair_norm = 2.0 * members * (members - 1)
    crps_value = lax.optimization_barrier(jnp.sum(skill_abs, axis=0)) / members - (lax.optimization_barrier(jnp.sum(spread_abs, axis=0)) - members * SMOOTH) / pair_norm
    loss = jnp.sum(area[None, :] * crps_value) / (VARS * GRID)
    field_grad = (area[None, None, :] * (skill_gap / skill_abs - spread_slope / (members - 1))).astype(jnp.bfloat16)
    return (loss, field_grad)
```

```python
import functools

import jax
import jax.numpy as jnp
from jax import lax
from jax.experimental import pallas as pl
from jax.experimental.pallas import tpu as pltpu
from jax.sharding import Mesh
from jax.sharding import PartitionSpec as P

SPACE = ("space_0", "space_1", "space_2")
MEMBER = ("member_0", "member_1")
SMOOTH2 = 0.0625
EPS = 1e-05
F32 = jnp.float32
BF16 = jnp.bfloat16
NEG = -1e30
VMEM = pl.BlockSpec(memory_space=pltpu.VMEM)

OFFSETS = (1, 7, 2, 6, 3, 5, 4)


def dot(a, b, ca, cb):
    return lax.dot_general(a, b, (((ca,), (cb,)), ((), ())), preferred_element_type=F32)


def place():
    return tuple(lax.axis_index(a) for a in MEMBER + SPACE)


def remote(src, dst, send, recv, device):
    return pltpu.make_async_remote_copy(
        src_ref=src,
        dst_ref=dst,
        send_sem=send,
        recv_sem=recv,
        device_id=device,
        device_id_type=pl.DeviceIdType.MESH,
    )


def at_y(me, step):
    yh, x, z, yl, c = me
    y = lax.rem(4 * yh + yl + 8 + step, 8)
    return (y // 4, x, z, lax.rem(y, 4), c)


def at_z(me, step):
    yh, x, z, yl, c = me
    return (yh, x, lax.rem(z + 8 + step, 8), yl, c)


def at_x(me, step):
    yh, x, z, yl, c = me
    return (yh, lax.rem(x + 4 + step, 4), z, yl, c)


def at_core(me):
    yh, x, z, yl, c = me
    return (yh, x, z, yl, 1 - c)


def at_block(me, step):
    yh, x, z, yl, c = me
    s = lax.rem(z * 8 + yl * 2 + c + 64 + step, 64)
    return (yh, x, s // 8, lax.rem(s, 8) // 2, lax.rem(s, 2))


def greet(devices):
    barrier = pltpu.get_barrier_semaphore()
    for d in devices:
        pl.semaphore_signal(barrier, inc=1, device_id=d, device_id_type=pl.DeviceIdType.MESH)
    return lambda: pl.semaphore_wait(barrier, len(devices))


def gather_kernel(
    wq, wk, wv, wo, wd, states, noise, rows,
    wall, halo, nhalo, nown,
    picked, npicked,
    zs, zr, ys, yr, cs, cr, hs, hr, ns, nr, xs, xr,
):
    me = place()
    yh, x, z, yl, c = me
    wait_all = greet(
        [at_z(me, o) for o in OFFSETS]
        + [at_y(me, 1), at_y(me, -1), at_y(me, 2), at_y(me, -2), at_core(me)]
        + [at_x(me, 1), at_x(me, 2), at_x(me, 3)]
        + [at_block(me, 1), at_block(me, -1)]
    )
    columns = pl.ds(pl.multiple_of(256 * x, 256), 256)
    mine = wall.at[z, yl, c]
    mine[:, 0:256] = wq[:, columns]
    mine[:, 256:512] = wk[:, columns]
    mine[:, 512:768] = wv[:, columns]
    mine[:, 768:896] = dot(wo[...], wd[...], 1, 1).astype(BF16)
    nown[x] = noise[...]
    chosen = (lax.broadcasted_iota(jnp.int32, (256, 256), 0) == rows[...]).astype(F32).astype(BF16)
    picked[...] = dot(chosen, states[...], 0, 0).astype(BF16).reshape(2, 128, 1024)
    sent_noise = dot(noise[...], chosen, 1, 0).astype(BF16)
    npicked[0] = sent_noise[:, 0:128]
    npicked[1] = sent_noise[:, 128:256]
    wait_all()

    started = []

    def go(copy):
        copy.start()
        started.append(copy)

    quarter = pl.ds(pl.multiple_of(32 * x, 32), 32)
    for i, (half, step) in enumerate(((1, 1), (0, -1))):
        go(remote(picked.at[half, quarter], halo.at[i, quarter], hs.at[i], hr.at[i], at_block(me, step)))
        go(remote(npicked.at[half], nhalo.at[x, i], ns.at[i], nr.at[i], at_block(me, step)))
    for o in OFFSETS:
        go(remote(mine, mine, zs.at[o], zr.at[o], at_z(me, o)))
    for t in (1, 2, 3):
        go(remote(nown.at[x], nown.at[x], xs.at[t, 0], xr.at[t, 0], at_x(me, t)))

    def y_steps(k):
        return (1, -1, 2 if k % 2 == 0 else -2)

    def forward_y(k, o):
        zk = lax.rem(z + 8 - o, 8)
        for t, step in enumerate(y_steps(k)):
            block = wall.at[zk, yl, c]
            go(remote(block, block, ys.at[k, t], yr.at[k, t], at_y(me, step)))

    def forward_core(k, o):
        zk = lax.rem(z + 8 - o, 8)
        for t, step in enumerate(y_steps(k)):
            landed = wall.at[zk, lax.rem(yl + 4 - step, 4), c]
            remote(landed, landed, ys.at[k, t], yr.at[k, t], at_y(me, -step)).wait_recv()
        both = wall.at[zk, :, c]
        go(remote(both, both, cs.at[k], cr.at[k], at_core(me)))

    def forward_x():
        for i, step in enumerate((1, -1)):
            part = halo.at[i, quarter]
            remote(part, part, hs.at[i], hr.at[i], at_block(me, -step)).wait_recv()
            part = nhalo.at[x, i]
            remote(part, part, ns.at[i], nr.at[i], at_block(me, -step)).wait_recv()
        for t in (1, 2, 3):
            go(remote(halo.at[:, quarter], halo.at[:, quarter], xs.at[t, 1], xr.at[t, 1], at_x(me, t)))
            go(remote(nhalo.at[x], nhalo.at[x], xs.at[t, 2], xr.at[t, 2], at_x(me, t)))

    order = (0,) + OFFSETS
    for k, o in enumerate(order):
        if o:
            landed = wall.at[lax.rem(z + 8 - o, 8), yl, c]
            remote(landed, landed, zs.at[o], zr.at[o], at_z(me, -o)).wait_recv()
        forward_y(k, o)
        if k == 3:
            forward_x()
        if k >= 2:
            forward_core(k - 2, order[k - 2])
    forward_core(6, order[6])
    forward_core(7, order[7])
    for k, o in enumerate(order):
        landed = wall.at[lax.rem(z + 8 - o, 8), :, 1 - c]
        remote(landed, landed, cs.at[k], cr.at[k], at_core(me)).wait_recv()
    for t in (1, 2, 3):
        other = lax.rem(x + 4 - t, 4)
        slot = nown.at[other]
        remote(slot, slot, xs.at[t, 0], xr.at[t, 0], at_x(me, -t)).wait_recv()
        slot = halo.at[:, pl.ds(pl.multiple_of(32 * other, 32), 32)]
        remote(slot, slot, xs.at[t, 1], xr.at[t, 1], at_x(me, -t)).wait_recv()
        slot = nhalo.at[other]
        remote(slot, slot, xs.at[t, 2], xr.at[t, 2], at_x(me, -t)).wait_recv()
    for copy in started:
        copy.wait_send()


def attend_kernel(
    wall, states, halo, nown, nhalo, gain, cond, edges,
    out,
    normed, counts, hidden, wvt, w2t, att,
):
    x = lax.axis_index(MEMBER[1])

    def normalise(values, at):
        v = values.astype(F32)
        center = v - jnp.mean(v, axis=1, keepdims=True)
        spread = jnp.mean(center * center, axis=1, keepdims=True)
        normed[pl.ds(at, 128), :] = center * lax.rsqrt(spread + EPS) * gain[...]

    normalise(halo[0], 0)
    normalise(states[0:128, :], 128)
    normalise(states[128:256, :], 256)
    normalise(halo[1], 384)
    row = lax.broadcasted_iota(jnp.int32, (512, 256), 0)
    total = jnp.zeros((512, 256), F32)
    for k in range(8):
        total = total + (row == edges[k : k + 1, :]).astype(F32)
    counts[...] = total
    weights = wall[...].reshape(1024, 896)
    wvt[...] = weights[:, 512:768].T
    pair = wall[pl.ds(2 * x, 2)].reshape(256, 896)
    w2t[...] = pair[:, 768:896].T
    lane = lax.broadcasted_iota(jnp.int32, (256, 256), 1) // 64

    def member(m, _):
        noises = (nhalo[m, 0], nown[m, :, 0:128], nown[m, :, 128:256], nhalo[m, 1])
        for i in range(4):
            terms = dot(noises[i], cond[...], 0, 0)
            rows = slice(128 * i, 128 * i + 128)
            hidden[rows, :] = (normed[rows, :] * (1.0 + terms[:, :1024]) + terms[:, 1024:]).astype(BF16)
        all_rows = hidden[...]
        w = wall[...].reshape(1024, 896)
        query = dot(hidden[128:384, :], w[:, 0:256], 1, 0).astype(BF16) * 0.125
        key = dot(all_rows, w[:, 256:512], 1, 0).astype(BF16)
        value_t = dot(wvt[...], all_rows, 1, 1).astype(BF16)
        for h in range(4):
            one = jnp.where(lane == h, query, jnp.zeros_like(query))
            scores = dot(key, one, 1, 1)
            count = counts[...]
            scores = jnp.where(count > 0.0, scores, NEG)
            top = jnp.max(scores, axis=0, keepdims=True)
            weight = jnp.exp(scores - top) * count
            below = jnp.sum(weight, axis=0, keepdims=True)
            above = dot(value_t[64 * h : 64 * h + 64, :], weight.astype(BF16), 1, 0)
            att[64 * h : 64 * h + 64, :] = (above / below).astype(BF16)
        out[m] = dot(w2t[...], att[...], 1, 0).astype(BF16)
        return 0

    lax.fori_loop(0, 4, member, 0)


def score_kernel(
    part, states, wd, dec_src, dec_weight, truth, area,
    grad, loss,
    got, mine, theirs, wide, tall, fields, made, l0, l1, l2, l3, b1, b2, b3,
    ps, pr, ys, yr, gs, gr, ls, lr,
):
    me = place()
    yh, x, z, yl, c = me
    plane = [
        (yh, lax.rem(x + dx, 4), z, yl, lax.rem(c + dc, 2))
        for dx in range(4)
        for dc in range(2)
        if dx or dc
    ]
    plane_from = [
        (yh, lax.rem(x + 4 - dx, 4), z, yl, lax.rem(c + dc, 2))
        for dx in range(4)
        for dc in range(2)
        if dx or dc
    ]
    wait_all = greet(
        plane + [at_z(me, o) for o in range(1, 8)] + [at_y(me, o) for o in range(1, 8)]
    )
    node = lax.broadcasted_iota(jnp.int32, (256, 1024), 0)
    select = jnp.zeros((256, 1024), F32)
    for k in range(3):
        select = select + jnp.where(node == dec_src[k : k + 1, :], dec_weight[k : k + 1, :], 0.0)
    wide[0] = select.astype(BF16)
    wide[1] = (select - wide[0].astype(F32)).astype(BF16)
    tall[...] = jnp.zeros_like(tall)
    tall[0:100, :] = truth[...].astype(F32)
    group = pl.ds(pl.multiple_of(32 * x, 32), 32)
    base = dot(wd[group, :], states[...], 1, 1)
    wait_all()

    started = []

    def go(copy):
        copy.start()
        started.append(copy)

    for t in (1, 2, 3):
        peer = at_x(me, t)
        rows = pl.ds(pl.multiple_of(32 * peer[1], 32), 32)
        go(remote(part.at[:, rows], got.at[t], ps.at[t], pr.at[t], peer))
    update = part[:, group, :].astype(F32)
    for t in (1, 2, 3):
        remote(got.at[t], got.at[t], ps.at[t], pr.at[t], at_x(me, -t)).wait_recv()
        update = update + got[t].astype(F32)
    mine[...] = update.astype(BF16)
    go(remote(mine, theirs, ys.at[0], yr.at[0], at_y(me, 4)))

    def decode(source, at):
        for m in range(4):
            whole = base + source[m].astype(F32)
            high = whole.astype(BF16)
            low = (whole - high.astype(F32)).astype(BF16)
            value = dot(high, wide[0], 1, 0) + dot(low, wide[0], 1, 0) + dot(high, wide[1], 1, 0)
            fields[at + m] = value.astype(BF16).astype(F32)

    decode(mine, 0)
    remote(theirs, theirs, ys.at[0], yr.at[0], at_y(me, 4)).wait_recv()
    decode(theirs, 4)

    valid = lax.broadcasted_iota(jnp.int32, (32, 128), 0) + 32 * x < 100

    def columns(i, carry):
        cols = pl.ds(pl.multiple_of(128 * i, 128), 128)
        a = area[:, cols]
        y = tall[group, cols]
        f = [fields[m, :, cols] for m in range(8)]
        slopes = [jnp.zeros((32, 128), F32) for _ in range(4)]
        spread = jnp.zeros((32, 128), F32)
        skill = jnp.zeros((32, 128), F32)
        for m in range(4):
            for n in range(m + 1, 8):
                d = f[m] - f[n]
                q = d * d + SMOOTH2
                r = lax.rsqrt(q)
                s = d * r
                slopes[m] = slopes[m] + s
                if n < 4:
                    slopes[n] = slopes[n] - s
                    spread = spread + 2.0 * (q * r)
                else:
                    spread = spread + q * r
        for m in range(4):
            d = f[m] - y
            q = d * d + SMOOTH2
            r = lax.rsqrt(q)
            skill = skill + q * r
            made[m, :, cols] = (a * (d * r - slopes[m] * (1.0 / 7.0))).astype(BF16)
        score = a * (skill * (1.0 / 8.0) - spread * (1.0 / 112.0))
        score = jnp.where(valid, score, 0.0)
        return carry + score

    total = lax.fori_loop(0, 8, columns, jnp.zeros((32, 128), F32))
    l0[...] = total[0:8] + total[8:16] + total[16:24] + total[24:32]

    for t, peer in enumerate(plane):
        go(remote(l0, b1.at[t], ls.at[0, t], lr.at[0, t], peer))
    for t in (1, 2, 3):
        peer = at_x(me, t)
        go(remote(made.at[peer[1]], grad.at[group], gs.at[t], gr.at[t], peer))
    grad[group, :] = made[x]

    def collect(here, inbox, stage, sources):
        value = here[...]
        for t, peer in enumerate(sources):
            remote(inbox.at[t], inbox.at[t], ls.at[stage, t], lr.at[stage, t], peer).wait_recv()
            value = value + inbox[t]
        return value

    l1[...] = collect(l0, b1, 0, plane_from)
    for t in range(7):
        go(remote(l1, b2.at[t], ls.at[1, t], lr.at[1, t], at_z(me, t + 1)))
    l2[...] = collect(l1, b2, 1, [at_z(me, -t) for t in range(1, 8)])
    for t in range(7):
        go(remote(l2, b3.at[t], ls.at[2, t], lr.at[2, t], at_y(me, t + 1)))
    value = collect(l2, b3, 2, [at_y(me, -t) for t in range(1, 8)])
    value = jnp.sum(jnp.sum(value, axis=0, keepdims=True), axis=1, keepdims=True)
    loss[...] = value * (1.0 / 6553600.0)
    for t in (1, 2, 3):
        peer = at_x(me, -t)
        rows = pl.ds(pl.multiple_of(32 * peer[1], 32), 32)
        remote(grad.at[rows], grad.at[rows], gs.at[t], gr.at[t], peer).wait_recv()
    for copy in started:
        copy.wait_send()


def dma(*shape):
    return pltpu.SemaphoreType.DMA(shape)


def per_device(
    node_states, noise, norm_gain, cond_weight, w_query, w_key, w_value, w_out,
    edge_src, send_rows, dec_src, dec_weight, w_decode, truth, area,
):
    decoder = jnp.pad(w_decode, ((0, 28), (0, 0)))
    wall, halo, nhalo, nown = pl.pallas_call(
        gather_kernel,
        out_shape=(
            jax.ShapeDtypeStruct((8, 4, 2, 16, 896), BF16),
            jax.ShapeDtypeStruct((2, 128, 1024), BF16),
            jax.ShapeDtypeStruct((4, 2, 16, 128), BF16),
            jax.ShapeDtypeStruct((4, 16, 256), BF16),
        ),
        in_specs=[VMEM] * 8,
        out_specs=(VMEM,) * 4,
        scratch_shapes=[
            pltpu.VMEM((2, 128, 1024), BF16),
            pltpu.VMEM((2, 16, 128), BF16),
            dma(8), dma(8), dma(8, 3), dma(8, 3), dma(8), dma(8), dma(2), dma(2), dma(2), dma(2),
            dma(4, 3), dma(4, 3),
        ],
        compiler_params=pltpu.CompilerParams(collective_id=0, has_side_effects=True),
        name="gather",
    )(w_query, w_key, w_value, w_out, decoder, node_states, noise[0], send_rows.reshape(1, 256))
    part = pl.pallas_call(
        attend_kernel,
        out_shape=jax.ShapeDtypeStruct((4, 128, 256), BF16),
        in_specs=[VMEM] * 8,
        out_specs=VMEM,
        scratch_shapes=[
            pltpu.VMEM((512, 1024), F32),
            pltpu.VMEM((512, 256), F32),
            pltpu.VMEM((512, 1024), BF16),
            pltpu.VMEM((256, 1024), BF16),
            pltpu.VMEM((128, 256), BF16),
            pltpu.VMEM((256, 256), BF16),
        ],
        compiler_params=pltpu.CompilerParams(vmem_limit_bytes=48 * 1024 * 1024),
        name="attend",
    )(wall, node_states, halo, nown, nhalo, norm_gain.reshape(1, 1024), cond_weight, edge_src)
    grad, loss = pl.pallas_call(
        score_kernel,
        out_shape=(
            jax.ShapeDtypeStruct((128, 1024), BF16),
            jax.ShapeDtypeStruct((1, 1), F32),
        ),
        in_specs=[VMEM] * 7,
        out_specs=(VMEM, VMEM),
        scratch_shapes=[
            pltpu.VMEM((4, 4, 32, 256), BF16),
            pltpu.VMEM((4, 32, 256), BF16),
            pltpu.VMEM((4, 32, 256), BF16),
            pltpu.VMEM((2, 256, 1024), BF16),
            pltpu.VMEM((128, 1024), F32),
            pltpu.VMEM((8, 32, 1024), F32),
            pltpu.VMEM((4, 32, 1024), BF16),
            pltpu.VMEM((8, 128), F32),
            pltpu.VMEM((8, 128), F32),
            pltpu.VMEM((8, 128), F32),
            pltpu.VMEM((8, 128), F32),
            pltpu.VMEM((7, 8, 128), F32),
            pltpu.VMEM((7, 8, 128), F32),
            pltpu.VMEM((7, 8, 128), F32),
            dma(4), dma(4), dma(1), dma(1), dma(4), dma(4), dma(3, 7), dma(3, 7),
        ],
        compiler_params=pltpu.CompilerParams(collective_id=1, has_side_effects=True),
        name="score",
    )(part, node_states, decoder, dec_src, dec_weight, truth, area.reshape(1, 1024))
    return loss[0, 0], grad[None, :100]


def solution(mesh):
    split = Mesh(mesh.devices.reshape(2, 4, 8, 4, 2), MEMBER + SPACE)
    return jax.shard_map(
        per_device,
        mesh=split,
        in_specs=(
            P(SPACE, None),
            P(MEMBER, None, SPACE),
            P(),
            P(),
            P(SPACE, None),
            P(SPACE, None),
            P(SPACE, None),
            P(SPACE, None),
            P(None, SPACE),
            P(SPACE),
            P(None, SPACE),
            P(None, SPACE),
            P(),
            P(None, SPACE),
            P(SPACE),
        ),
        out_specs=(P(), P(MEMBER, None, SPACE)),
        check_vma=False,
    )
```

```python
import functools

import jax
import jax.numpy as jnp
from jax import lax
from jax.experimental import pallas as pl
from jax.experimental.pallas import tpu as pltpu
from jax.sharding import Mesh
from jax.sharding import PartitionSpec as P

SPACE = ("space_0", "space_1", "space_2")
MEMBER = ("member_0", "member_1")
SMOOTH2 = 0.0625
EPS = 1e-05
F32 = jnp.float32
BF16 = jnp.bfloat16
NEG = -1e30
VMEM = pl.BlockSpec(memory_space=pltpu.VMEM)

OFFSETS = (1, 7, 2, 6, 3, 5, 4)


def dot(a, b, ca, cb):
    return lax.dot_general(a, b, (((ca,), (cb,)), ((), ())), preferred_element_type=F32)


def place():
    return tuple(lax.axis_index(a) for a in MEMBER + SPACE)


def remote(src, dst, send, recv, device):
    return pltpu.make_async_remote_copy(
        src_ref=src,
        dst_ref=dst,
        send_sem=send,
        recv_sem=recv,
        device_id=device,
        device_id_type=pl.DeviceIdType.MESH,
    )


def at_y(me, step):
    yh, x, z, yl, c = me
    y = lax.rem(4 * yh + yl + 8 + step, 8)
    return (y // 4, x, z, lax.rem(y, 4), c)


def at_z(me, step):
    yh, x, z, yl, c = me
    return (yh, x, lax.rem(z + 8 + step, 8), yl, c)


def at_x(me, step):
    yh, x, z, yl, c = me
    return (yh, lax.rem(x + 4 + step, 4), z, yl, c)


def at_core(me):
    yh, x, z, yl, c = me
    return (yh, x, z, yl, 1 - c)


def at_block(me, step):
    yh, x, z, yl, c = me
    s = lax.rem(z * 8 + yl * 2 + c + 64 + step, 64)
    return (yh, x, s // 8, lax.rem(s, 8) // 2, lax.rem(s, 2))


def greet(devices):
    barrier = pltpu.get_barrier_semaphore()
    for d in devices:
        pl.semaphore_signal(barrier, inc=1, device_id=d, device_id_type=pl.DeviceIdType.MESH)
    return lambda: pl.semaphore_wait(barrier, len(devices))


def step_kernel(
    wq, wk, wv, wo, states_in, noise_in, rows_in, gain_in, cond_in, edges_in, wd_in,
    source_in, weight_in, truth_in, area_in,
    grad, loss,
    states, noise, rows, gain, cond, edges, wd, source, weight, truth, area, wo_here,
    wall, halo, nhalo, nown, picked, npicked,
    normed, counts, hidden, wvt, w2t, att,
    part, got, mine, theirs, wide, tall, fields, slopes, scores, made, l0, l1, l2, b1, b2, b3,
    fetch, zs, zr, ys, yr, cs, cr, hs, hr, ns, nr, xs, xr, ps, pr, fs, fr, gs, gr, ls, lr,
):
    me = place()
    yh, x, z, yl, c = me
    plane = [
        (yh, lax.rem(x + dx, 4), z, yl, lax.rem(c + dc, 2))
        for dx in range(4)
        for dc in range(2)
        if dx or dc
    ]
    plane_from = [
        (yh, lax.rem(x + 4 - dx, 4), z, yl, lax.rem(c + dc, 2))
        for dx in range(4)
        for dc in range(2)
        if dx or dc
    ]
    wait_all = greet(
        [at_z(me, o) for o in OFFSETS]
        + [at_y(me, o) for o in range(1, 8)]
        + plane
        + [at_block(me, 1), at_block(me, -1)]
    )
    columns = pl.ds(pl.multiple_of(256 * x, 256), 256)
    own = wall.at[z, yl, c]
    fetches = [
        pltpu.make_async_copy(a, b, fetch.at[i])
        for i, (a, b) in enumerate(
            (
                (rows_in, rows),
                (states_in, states),
                (noise_in, noise),
                (noise_in, nown.at[x]),
                (wo, wo_here),
                (wd_in, wd),
                (wq.at[:, columns], own.at[:, 0:256]),
                (wk.at[:, columns], own.at[:, 256:512]),
                (wv.at[:, columns], own.at[:, 512:768]),
                (gain_in, gain),
                (cond_in, cond),
                (edges_in, edges),
                (source_in, source),
                (weight_in, weight),
                (truth_in, truth),
                (area_in, area),
            )
        )
    ]
    for f in fetches:
        f.start()
    for f in fetches[:3]:
        f.wait()
    chosen = (lax.broadcasted_iota(jnp.int32, (256, 256), 0) == rows[...]).astype(F32).astype(BF16)
    picked[...] = dot(chosen, states[...], 0, 0).astype(BF16).reshape(2, 128, 1024)
    sent_noise = dot(noise[...], chosen, 1, 0).astype(BF16)
    npicked[0] = sent_noise[:, 0:128]
    npicked[1] = sent_noise[:, 128:256]
    for f in fetches[3:9]:
        f.wait()
    wall[z, yl, c, :, 768:868] = dot(wo_here[...], wd[...], 1, 1).astype(BF16)
    wall[z, yl, c, :, 868:896] = jnp.zeros((16, 28), BF16)
    wait_all()

    started = []

    def go(copy):
        copy.start()
        started.append(copy)

    quarter = pl.ds(pl.multiple_of(32 * x, 32), 32)
    for i, (half, step) in enumerate(((1, 1), (0, -1))):
        go(remote(picked.at[half, quarter], halo.at[i, quarter], hs.at[i], hr.at[i], at_block(me, step)))
        go(remote(npicked.at[half], nhalo.at[x, i], ns.at[i], nr.at[i], at_block(me, step)))
    for o in OFFSETS:
        go(remote(own, own, zs.at[o], zr.at[o], at_z(me, o)))
    for t in (1, 2, 3):
        go(remote(nown.at[x], nown.at[x], xs.at[t, 0], xr.at[t, 0], at_x(me, t)))

    def y_steps(k):
        return (1, -1, 2 if k % 2 == 0 else -2)

    order = (0,) + OFFSETS

    def forward_y(k):
        zk = lax.rem(z + 8 - order[k], 8)
        block = wall.at[zk, yl, c]
        if k:
            remote(block, block, zs.at[order[k]], zr.at[order[k]], at_z(me, -order[k])).wait_recv()
        for t, step in enumerate(y_steps(k)):
            go(remote(block, block, ys.at[k, t], yr.at[k, t], at_y(me, step)))

    def forward_core(k):
        zk = lax.rem(z + 8 - order[k], 8)
        for t, step in enumerate(y_steps(k)):
            landed = wall.at[zk, lax.rem(yl + 4 - step, 4), c]
            remote(landed, landed, ys.at[k, t], yr.at[k, t], at_y(me, -step)).wait_recv()
        both = wall.at[zk, :, c]
        go(remote(both, both, cs.at[k], cr.at[k], at_core(me)))

    def forward_x():
        for i, step in enumerate((1, -1)):
            slot = halo.at[i, quarter]
            remote(slot, slot, hs.at[i], hr.at[i], at_block(me, -step)).wait_recv()
            slot = nhalo.at[x, i]
            remote(slot, slot, ns.at[i], nr.at[i], at_block(me, -step)).wait_recv()
        for t in (1, 2, 3):
            go(remote(halo.at[:, quarter], halo.at[:, quarter], xs.at[t, 1], xr.at[t, 1], at_x(me, t)))
            go(remote(nhalo.at[x], nhalo.at[x], xs.at[t, 2], xr.at[t, 2], at_x(me, t)))

    def normalise(values, at):
        v = values.astype(F32)
        center = v - jnp.mean(v, axis=1, keepdims=True)
        spread = jnp.mean(center * center, axis=1, keepdims=True)
        normed[at : at + 128, :] = center * lax.rsqrt(spread + EPS) * gain[...]

    def condition(i, noises):
        rows = slice(128 * i, 128 * i + 128)
        for m in range(4):
            terms = dot(noises(m), cond[...], 0, 0)
            hidden[m, rows, :] = (normed[rows, :] * (1.0 + terms[:, :1024]) + terms[:, 1024:]).astype(BF16)

    forward_y(0)
    for f in fetches[9:]:
        f.wait()
    normalise(states[0:128, :], 128)
    forward_y(1)
    forward_y(2)
    normalise(states[128:256, :], 256)
    forward_y(3)
    forward_y(4)
    forward_x()
    for part_of in range(2):
        row = lax.broadcasted_iota(jnp.int32, (256, 256), 0) + 256 * part_of
        total = jnp.zeros((256, 256), F32)
        for k in range(8):
            total = total + (row == edges[k : k + 1, :]).astype(F32)
        counts[256 * part_of : 256 * part_of + 256, :] = total
    forward_y(5)
    forward_y(6)
    forward_y(7)
    forward_core(0)
    forward_core(1)
    for t in (1, 2, 3):
        other = lax.rem(x + 4 - t, 4)
        slot = nown.at[other]
        remote(slot, slot, xs.at[t, 0], xr.at[t, 0], at_x(me, -t)).wait_recv()
    condition(1, lambda m: nown[m, :, 0:128])
    forward_core(2)
    condition(2, lambda m: nown[m, :, 128:256])
    forward_core(3)
    for t in (1, 2, 3):
        other = lax.rem(x + 4 - t, 4)
        slot = halo.at[:, pl.ds(pl.multiple_of(32 * other, 32), 32)]
        remote(slot, slot, xs.at[t, 1], xr.at[t, 1], at_x(me, -t)).wait_recv()
        slot = nhalo.at[other]
        remote(slot, slot, xs.at[t, 2], xr.at[t, 2], at_x(me, -t)).wait_recv()
    normalise(halo[0], 0)
    condition(0, lambda m: nhalo[m, 0])
    forward_core(4)
    normalise(halo[1], 384)
    condition(3, lambda m: nhalo[m, 1])
    forward_core(5)
    node = lax.broadcasted_iota(jnp.int32, (256, 1024), 0)
    select = jnp.zeros((256, 1024), F32)
    for k in range(3):
        select = select + jnp.where(node == source[k : k + 1, :], weight[k : k + 1, :], 0.0)
    wide[0] = select.astype(BF16)
    wide[1] = (select - wide[0].astype(F32)).astype(BF16)
    forward_core(6)
    tall[0:100, :] = truth[...].astype(F32)
    tall[100:128, :] = jnp.zeros((28, 1024), F32)
    base = dot(wd[...], states[...], 1, 1)
    scores[0:100, 0:256] = base
    scores[100:128, 0:256] = jnp.zeros((28, 256), F32)
    forward_core(7)
    for k, o in enumerate(order):
        landed = wall.at[lax.rem(z + 8 - o, 8), :, 1 - c]
        remote(landed, landed, cs.at[k], cr.at[k], at_core(me)).wait_recv()

    wvt[...] = wall[...].reshape(1024, 896)[:, 512:768].T
    w2t[...] = wall[pl.ds(2 * x, 2)].reshape(256, 896)[:, 768:896].T
    lane = lax.broadcasted_iota(jnp.int32, (256, 256), 1) // 64
    group = quarter

    def to_x(m, t):
        peer = at_x(me, t)
        there = pl.ds(pl.multiple_of(32 * peer[1], 32), 32)
        return remote(part.at[m, there], got.at[m, t], ps.at[m, t], pr.at[m, t], peer)

    def to_other(m):
        return remote(mine.at[m], theirs.at[m], fs.at[m], fr.at[m], at_y(me, 4))

    def combine(m):
        update = part[m, group, :].astype(F32)
        for t in (1, 2, 3):
            remote(got.at[m, t], got.at[m, t], ps.at[m, t], pr.at[m, t], at_x(me, -t)).wait_recv()
            update = update + got[m, t].astype(F32)
        mine[m] = update.astype(BF16)
        to_other(m).start()

    def member(m, _):
        all_rows = hidden[m]
        w = wall[...].reshape(1024, 896)
        query = dot(hidden[m, 128:384, :], w[:, 0:256], 1, 0).astype(BF16) * 0.125
        key = dot(all_rows, w[:, 256:512], 1, 0).astype(BF16)
        value_t = dot(wvt[...], all_rows, 1, 1).astype(BF16)
        for h in range(4):
            one = jnp.where(lane == h, query, jnp.zeros_like(query))
            score = dot(key, one, 1, 1)
            count = counts[...]
            score = jnp.where(count > 0.0, score, NEG)
            top = jnp.max(score, axis=0, keepdims=True)
            share = jnp.exp(score - top) * count
            below = jnp.sum(share, axis=0, keepdims=True)
            above = dot(value_t[64 * h : 64 * h + 64, :], share.astype(BF16), 1, 0)
            att[64 * h : 64 * h + 64, :] = (above / below).astype(BF16)
        part[m] = dot(w2t[...], att[...], 1, 0).astype(BF16)
        for t in (1, 2, 3):
            to_x(m, t).start()

        @pl.when(m > 0)
        def _():
            combine(m - 1)

        return 0

    lax.fori_loop(0, 4, member, 0)
    combine(3)
    base = scores[group, 0:256]

    def decode(held, at):
        whole = (base[None] + held[...].astype(F32)).reshape(128, 256)
        high = whole.astype(BF16)
        low = (whole - high.astype(F32)).astype(BF16)
        both = dot(jnp.concatenate([high, low], axis=0), wide[0], 1, 0)
        value = both[0:128] + both[128:256] + dot(high, wide[1], 1, 0)
        fields[at : at + 4] = value.astype(BF16).astype(F32).reshape(4, 32, 1024)

    decode(mine, 0)
    valid = lax.broadcasted_iota(jnp.int32, (32, 128), 0) + 32 * x < 100

    def inner(i, _):
        cols = pl.ds(pl.multiple_of(128 * i, 128), 128)
        y = tall[group, cols]
        f = [fields[m, :, cols] for m in range(4)]
        slope = [jnp.zeros((32, 128), F32) for _ in range(4)]
        spread = jnp.zeros((32, 128), F32)
        skill = jnp.zeros((32, 128), F32)
        for m in range(4):
            for n in range(m + 1, 4):
                d = f[m] - f[n]
                q = d * d + SMOOTH2
                r = lax.rsqrt(q)
                s = d * r
                slope[m] = slope[m] + s
                slope[n] = slope[n] - s
                spread = spread + q * r
        for m in range(4):
            d = f[m] - y
            q = d * d + SMOOTH2
            r = lax.rsqrt(q)
            skill = skill + q * r
            slopes[m, :, cols] = d * r - slope[m] * (1.0 / 7.0)
        scores[0:32, cols] = skill * (1.0 / 8.0) - spread * (2.0 / 112.0)
        return 0

    lax.fori_loop(0, 8, inner, 0)
    for m in range(4):
        remote(theirs.at[m], theirs.at[m], fs.at[m], fr.at[m], at_y(me, 4)).wait_recv()
    decode(theirs, 4)

    def across(i, carry):
        cols = pl.ds(pl.multiple_of(128 * i, 128), 128)
        a = area[:, cols]
        f = [fields[m, :, cols] for m in range(8)]
        spread = jnp.zeros((32, 128), F32)
        for m in range(4):
            slope = jnp.zeros((32, 128), F32)
            for n in range(4, 8):
                d = f[m] - f[n]
                q = d * d + SMOOTH2
                r = lax.rsqrt(q)
                slope = slope + d * r
                spread = spread + q * r
            made[m, :, cols] = (a * (slopes[m, :, cols] - slope * (1.0 / 7.0))).astype(BF16)
        score = a * (scores[0:32, cols] - spread * (1.0 / 112.0))
        return carry + jnp.where(valid, score, 0.0)

    total = lax.fori_loop(0, 8, across, jnp.zeros((32, 128), F32))
    l0[...] = total[0:8] + total[8:16] + total[16:24] + total[24:32]

    for t, peer in enumerate(plane):
        go(remote(l0, b1.at[t], ls.at[0, t], lr.at[0, t], peer))
    for t in (1, 2, 3):
        peer = at_x(me, t)
        go(remote(made.at[peer[1]], grad.at[group], gs.at[t], gr.at[t], peer))
    grad[group, :] = made[x]

    def collect(here, inbox, stage, sources):
        value = here[...]
        for t, peer in enumerate(sources):
            remote(inbox.at[t], inbox.at[t], ls.at[stage, t], lr.at[stage, t], peer).wait_recv()
            value = value + inbox[t]
        return value

    l1[...] = collect(l0, b1, 0, plane_from)
    for t in range(7):
        go(remote(l1, b2.at[t], ls.at[1, t], lr.at[1, t], at_z(me, t + 1)))
    l2[...] = collect(l1, b2, 1, [at_z(me, -t) for t in range(1, 8)])
    for t in range(7):
        go(remote(l2, b3.at[t], ls.at[2, t], lr.at[2, t], at_y(me, t + 1)))
    value = collect(l2, b3, 2, [at_y(me, -t) for t in range(1, 8)])
    value = jnp.sum(jnp.sum(value, axis=0, keepdims=True), axis=1, keepdims=True)
    loss[...] = value * (1.0 / 6553600.0)
    for t in (1, 2, 3):
        peer = at_x(me, -t)
        there = pl.ds(pl.multiple_of(32 * peer[1], 32), 32)
        remote(grad.at[there], grad.at[there], gs.at[t], gr.at[t], peer).wait_recv()
    for copy in started:
        copy.wait_send()
    for m in range(4):
        for t in (1, 2, 3):
            to_x(m, t).wait_send()
        to_other(m).wait_send()


def dma(*shape):
    return pltpu.SemaphoreType.DMA(shape)


def per_device(
    node_states, noise, norm_gain, cond_weight, w_query, w_key, w_value, w_out,
    edge_src, send_rows, dec_src, dec_weight, w_decode, truth, area,
):
    grad, loss = pl.pallas_call(
        step_kernel,
        out_shape=(
            jax.ShapeDtypeStruct((128, 1024), BF16),
            jax.ShapeDtypeStruct((1, 1), F32),
        ),
        in_specs=[pl.BlockSpec(memory_space=pl.ANY)] * 15,
        out_specs=(VMEM, VMEM),
        scratch_shapes=[
            pltpu.VMEM((256, 1024), BF16),
            pltpu.VMEM((16, 256), BF16),
            pltpu.VMEM((1, 256), jnp.int32),
            pltpu.VMEM((1, 1024), F32),
            pltpu.VMEM((16, 2048), BF16),
            pltpu.VMEM((8, 256), jnp.int32),
            pltpu.VMEM((100, 1024), BF16),
            pltpu.VMEM((3, 1024), jnp.int32),
            pltpu.VMEM((3, 1024), F32),
            pltpu.VMEM((100, 1024), BF16),
            pltpu.VMEM((1, 1024), F32),
            pltpu.VMEM((16, 1024), BF16),
            pltpu.VMEM((8, 4, 2, 16, 896), BF16),
            pltpu.VMEM((2, 128, 1024), BF16),
            pltpu.VMEM((4, 2, 16, 128), BF16),
            pltpu.VMEM((4, 16, 256), BF16),
            pltpu.VMEM((2, 128, 1024), BF16),
            pltpu.VMEM((2, 16, 128), BF16),
            pltpu.VMEM((512, 1024), F32),
            pltpu.VMEM((512, 256), F32),
            pltpu.VMEM((4, 512, 1024), BF16),
            pltpu.VMEM((256, 1024), BF16),
            pltpu.VMEM((128, 256), BF16),
            pltpu.VMEM((256, 256), BF16),
            pltpu.VMEM((4, 128, 256), BF16),
            pltpu.VMEM((4, 4, 32, 256), BF16),
            pltpu.VMEM((4, 32, 256), BF16),
            pltpu.VMEM((4, 32, 256), BF16),
            pltpu.VMEM((2, 256, 1024), BF16),
            pltpu.VMEM((128, 1024), F32),
            pltpu.VMEM((8, 32, 1024), F32),
            pltpu.VMEM((4, 32, 1024), F32),
            pltpu.VMEM((128, 1024), F32),
            pltpu.VMEM((4, 32, 1024), BF16),
            pltpu.VMEM((8, 128), F32),
            pltpu.VMEM((8, 128), F32),
            pltpu.VMEM((8, 128), F32),
            pltpu.VMEM((7, 8, 128), F32),
            pltpu.VMEM((7, 8, 128), F32),
            pltpu.VMEM((7, 8, 128), F32),
            dma(16),
            dma(8), dma(8), dma(8, 3), dma(8, 3), dma(8), dma(8), dma(2), dma(2), dma(2), dma(2),
            dma(4, 3), dma(4, 3), dma(4, 4), dma(4, 4), dma(4), dma(4), dma(4), dma(4),
            dma(3, 7), dma(3, 7),
        ],
        compiler_params=pltpu.CompilerParams(collective_id=0, has_side_effects=True),
        name="step",
    )(
        w_query, w_key, w_value, w_out, node_states, noise[0], send_rows.reshape(1, 256),
        norm_gain.reshape(1, 1024), cond_weight, edge_src, w_decode,
        dec_src, dec_weight, truth, area.reshape(1, 1024),
    )
    return loss[0, 0], grad[None, :100]


def solution(mesh):
    split = Mesh(mesh.devices.reshape(2, 4, 8, 4, 2), MEMBER + SPACE)
    return jax.shard_map(
        per_device,
        mesh=split,
        in_specs=(
            P(SPACE, None),
            P(MEMBER, None, SPACE),
            P(),
            P(),
            P(SPACE, None),
            P(SPACE, None),
            P(SPACE, None),
            P(SPACE, None),
            P(None, SPACE),
            P(SPACE),
            P(None, SPACE),
            P(None, SPACE),
            P(),
            P(None, SPACE),
            P(SPACE),
        ),
        out_specs=(P(), P(MEMBER, None, SPACE)),
        check_vma=False,
    )
```

```python
import functools

import jax
import jax.numpy as jnp
from jax import lax
from jax.experimental import pallas as pl
from jax.experimental.pallas import tpu as pltpu
from jax.sharding import Mesh
from jax.sharding import PartitionSpec as P

SPACE = ("space_0", "space_1", "space_2")
MEMBER = ("member_0", "member_1")
SMOOTH2 = 0.0625
EPS = 1e-05
F32 = jnp.float32
BF16 = jnp.bfloat16
NEG = -1e30
VMEM = pl.BlockSpec(memory_space=pltpu.VMEM)

OFFSETS = (1, 7, 2, 6, 3, 5, 4)


def dot(a, b, ca, cb):
    return lax.dot_general(a, b, (((ca,), (cb,)), ((), ())), preferred_element_type=F32)


def place():
    return tuple(lax.axis_index(a) for a in MEMBER + SPACE)


def remote(src, dst, send, recv, device):
    return pltpu.make_async_remote_copy(
        src_ref=src,
        dst_ref=dst,
        send_sem=send,
        recv_sem=recv,
        device_id=device,
        device_id_type=pl.DeviceIdType.MESH,
    )


def at_y(me, step):
    yh, x, z, yl, c = me
    y = lax.rem(4 * yh + yl + 8 + step, 8)
    return (y // 4, x, z, lax.rem(y, 4), c)


def at_z(me, step):
    yh, x, z, yl, c = me
    return (yh, x, lax.rem(z + 8 + step, 8), yl, c)


def at_x(me, step):
    yh, x, z, yl, c = me
    return (yh, lax.rem(x + 4 + step, 4), z, yl, c)


def at_core(me):
    yh, x, z, yl, c = me
    return (yh, x, z, yl, 1 - c)


def at_block(me, step):
    yh, x, z, yl, c = me
    s = lax.rem(z * 8 + yl * 2 + c + 64 + step, 64)
    return (yh, x, s // 8, lax.rem(s, 8) // 2, lax.rem(s, 2))


def greet(devices):
    barrier = pltpu.get_barrier_semaphore()
    for d in devices:
        pl.semaphore_signal(barrier, inc=1, device_id=d, device_id_type=pl.DeviceIdType.MESH)
    return lambda: pl.semaphore_wait(barrier, len(devices))


def step_kernel(
    wq, wk, wv, wo, states_in, noise_in, rows_in, gain_in, cond_in, edges_in, wd_in,
    source_in, weight_in, truth_in, area_in,
    grad, loss,
    states, noise, rows, gain, cond, edges, wd, source, weight, truth, area, wo_here,
    wall, halo, nhalo, nown, picked, npicked,
    normed, counts, hidden, wvt, w2t, att,
    part, got, mine, theirs, wide, tall, fields, slopes, scores, made, l0, l1, b1, b2,
    fetch, zs, zr, ys, yr, cs, cr, hs, hr, ns, nr, xs, xr, ps, pr, fs, fr, gs, gr, ls, lr, zs2, zr2,
):
    me = place()
    yh, x, z, yl, c = me
    spots = [(dx, dc, dy) for dy in (2, 1, -1, 0) for dx in range(4) for dc in range(2) if dx or dc or dy]

    def near(dx, dc, dy):
        yh_, _, _, yl_, _ = at_y(me, dy)
        return (yh_, lax.rem(x + 4 + dx, 4), z, yl_, lax.rem(c + dc, 2))

    wait_all = greet(
        [at_z(me, o) for o in OFFSETS]
        + [at_y(me, o) for o in (1, -1, 2, -2, 4)]
        + [at_core(me)]
        + [at_x(me, o) for o in (1, 2, 3)]
        + [at_block(me, 1), at_block(me, -1)]
        + [near(-dx, dc, -dy) for dx, dc, dy in spots]
    )
    columns = pl.ds(pl.multiple_of(256 * x, 256), 256)
    own = wall.at[z, yl, c]
    fetches = [
        pltpu.make_async_copy(a, b, fetch.at[i])
        for i, (a, b) in enumerate(
            (
                (rows_in, rows),
                (states_in, states),
                (noise_in, noise),
                (noise_in, nown.at[x]),
                (wo, wo_here),
                (wd_in, wd),
                (wq.at[:, columns], own.at[:, 0:256]),
                (wk.at[:, columns], own.at[:, 256:512]),
                (wv.at[:, columns], own.at[:, 512:768]),
                (gain_in, gain),
                (cond_in, cond),
                (edges_in, edges),
                (source_in, source),
                (weight_in, weight),
                (truth_in, truth),
                (area_in, area),
            )
        )
    ]
    for f in fetches:
        f.start()
    for f in fetches[:3]:
        f.wait()
    chosen = (lax.broadcasted_iota(jnp.int32, (256, 256), 0) == rows[...]).astype(F32).astype(BF16)
    picked[...] = dot(chosen, states[...], 0, 0).astype(BF16).reshape(2, 128, 1024)
    sent_noise = dot(noise[...], chosen, 1, 0).astype(BF16)
    npicked[0] = sent_noise[:, 0:128]
    npicked[1] = sent_noise[:, 128:256]
    for f in fetches[3:9]:
        f.wait()
    wall[z, yl, c, :, 768:868] = dot(wo_here[...], wd[...], 1, 1).astype(BF16)
    wall[z, yl, c, :, 868:896] = jnp.zeros((16, 28), BF16)
    wait_all()

    started = []

    def go(copy):
        copy.start()
        started.append(copy)

    quarter = pl.ds(pl.multiple_of(32 * x, 32), 32)
    for i, (half, step) in enumerate(((1, 1), (0, -1))):
        go(remote(picked.at[half, quarter], halo.at[i, quarter], hs.at[i], hr.at[i], at_block(me, step)))
        go(remote(npicked.at[half], nhalo.at[x, i], ns.at[i], nr.at[i], at_block(me, step)))
    for o in OFFSETS:
        go(remote(own, own, zs.at[o], zr.at[o], at_z(me, o)))
    for t in (1, 2, 3):
        go(remote(nown.at[x], nown.at[x], xs.at[t, 0], xr.at[t, 0], at_x(me, t)))

    def y_steps(k):
        return (1, -1, 2 if k % 2 == 0 else -2)

    order = (0,) + OFFSETS

    def forward_y(k):
        zk = lax.rem(z + 8 - order[k], 8)
        block = wall.at[zk, yl, c]
        if k:
            remote(block, block, zs.at[order[k]], zr.at[order[k]], at_z(me, -order[k])).wait_recv()
        for t, step in enumerate(y_steps(k)):
            go(remote(block, block, ys.at[k, t], yr.at[k, t], at_y(me, step)))

    def forward_core(k):
        zk = lax.rem(z + 8 - order[k], 8)
        for t, step in enumerate(y_steps(k)):
            landed = wall.at[zk, lax.rem(yl + 4 - step, 4), c]
            remote(landed, landed, ys.at[k, t], yr.at[k, t], at_y(me, -step)).wait_recv()
        both = wall.at[zk, :, c]
        go(remote(both, both, cs.at[k], cr.at[k], at_core(me)))

    def forward_x():
        for i, step in enumerate((1, -1)):
            slot = halo.at[i, quarter]
            remote(slot, slot, hs.at[i], hr.at[i], at_block(me, -step)).wait_recv()
            slot = nhalo.at[x, i]
            remote(slot, slot, ns.at[i], nr.at[i], at_block(me, -step)).wait_recv()
        for t in (1, 2, 3):
            go(remote(halo.at[:, quarter], halo.at[:, quarter], xs.at[t, 1], xr.at[t, 1], at_x(me, t)))
            go(remote(nhalo.at[x], nhalo.at[x], xs.at[t, 2], xr.at[t, 2], at_x(me, t)))

    def normalise(values, at):
        v = values.astype(F32)
        center = v - jnp.mean(v, axis=1, keepdims=True)
        spread = jnp.mean(center * center, axis=1, keepdims=True)
        normed[at : at + 128, :] = center * lax.rsqrt(spread + EPS) * gain[...]

    def condition(i, noises):
        rows = slice(128 * i, 128 * i + 128)
        for m in range(4):
            terms = dot(noises(m), cond[...], 0, 0)
            hidden[m, rows, :] = (normed[rows, :] * (1.0 + terms[:, :1024]) + terms[:, 1024:]).astype(BF16)

    forward_y(0)
    for f in fetches[9:]:
        f.wait()
    normalise(states[0:128, :], 128)
    forward_y(1)
    forward_y(2)
    normalise(states[128:256, :], 256)
    forward_y(3)
    forward_y(4)
    forward_x()
    for part_of in range(2):
        row = lax.broadcasted_iota(jnp.int32, (256, 256), 0) + 256 * part_of
        total = jnp.zeros((256, 256), F32)
        for k in range(8):
            total = total + (row == edges[k : k + 1, :]).astype(F32)
        counts[256 * part_of : 256 * part_of + 256, :] = jnp.where(
            total > 0.0, jnp.log(jnp.maximum(total, 1.0)), NEG
        )
    forward_y(5)
    forward_y(6)
    forward_y(7)
    forward_core(0)
    forward_core(1)
    for t in (1, 2, 3):
        other = lax.rem(x + 4 - t, 4)
        slot = nown.at[other]
        remote(slot, slot, xs.at[t, 0], xr.at[t, 0], at_x(me, -t)).wait_recv()
    condition(1, lambda m: nown[m, :, 0:128])
    forward_core(2)
    condition(2, lambda m: nown[m, :, 128:256])
    forward_core(3)
    for t in (1, 2, 3):
        other = lax.rem(x + 4 - t, 4)
        slot = halo.at[:, pl.ds(pl.multiple_of(32 * other, 32), 32)]
        remote(slot, slot, xs.at[t, 1], xr.at[t, 1], at_x(me, -t)).wait_recv()
        slot = nhalo.at[other]
        remote(slot, slot, xs.at[t, 2], xr.at[t, 2], at_x(me, -t)).wait_recv()
    normalise(halo[0], 0)
    condition(0, lambda m: nhalo[m, 0])
    forward_core(4)
    normalise(halo[1], 384)
    condition(3, lambda m: nhalo[m, 1])
    forward_core(5)
    node = lax.broadcasted_iota(jnp.int32, (256, 1024), 0)
    select = jnp.zeros((256, 1024), F32)
    for k in range(3):
        select = select + jnp.where(node == source[k : k + 1, :], weight[k : k + 1, :], 0.0)
    wide[0] = select.astype(BF16)
    wide[1] = (select - wide[0].astype(F32)).astype(BF16)
    forward_core(6)
    tall[0:100, :] = truth[...].astype(F32)
    tall[100:128, :] = jnp.zeros((28, 1024), F32)
    base = dot(wd[...], states[...], 1, 1)
    scores[0:100, 0:256] = base
    scores[100:128, 0:256] = jnp.zeros((28, 256), F32)
    forward_core(7)
    for k, o in enumerate(order):
        landed = wall.at[lax.rem(z + 8 - o, 8), :, 1 - c]
        remote(landed, landed, cs.at[k], cr.at[k], at_core(me)).wait_recv()

    wvt[...] = wall[...].reshape(1024, 896)[:, 512:768].T
    w2t[...] = wall[pl.ds(2 * x, 2)].reshape(256, 896)[:, 768:896].T
    lane = lax.broadcasted_iota(jnp.int32, (256, 256), 1) // 64
    group = quarter

    def to_x(m, t):
        peer = at_x(me, t)
        there = pl.ds(pl.multiple_of(32 * peer[1], 32), 32)
        return remote(part.at[m, there], got.at[m, t], ps.at[m, t], pr.at[m, t], peer)

    def to_other(m):
        return remote(mine.at[m], theirs.at[m], fs.at[m], fr.at[m], at_y(me, 4))

    def combine(m):
        update = part[m, group, :].astype(F32)
        for t in (1, 2, 3):
            remote(got.at[m, t], got.at[m, t], ps.at[m, t], pr.at[m, t], at_x(me, -t)).wait_recv()
            update = update + got[m, t].astype(F32)
        mine[m] = update.astype(BF16)
        to_other(m).start()

    def member(m, _):
        all_rows = hidden[m]
        w = wall[...].reshape(1024, 896)
        query = dot(hidden[m, 128:384, :], w[:, 0:256], 1, 0).astype(BF16) * 0.125
        key = dot(all_rows, w[:, 256:512], 1, 0).astype(BF16)
        value_t = dot(wvt[...], all_rows, 1, 1).astype(BF16)
        for h in range(4):
            one = jnp.where(lane == h, query, jnp.zeros_like(query))
            score = dot(key, one, 1, 1) + counts[...]
            top = jnp.max(score, axis=0, keepdims=True)
            share = jnp.exp(score - top)
            below = jnp.sum(share, axis=0, keepdims=True)
            above = dot(value_t[64 * h : 64 * h + 64, :], share.astype(BF16), 1, 0)
            att[64 * h : 64 * h + 64, :] = (above / below).astype(BF16)
        part[m] = dot(w2t[...], att[...], 1, 0).astype(BF16)
        for t in (1, 2, 3):
            to_x(m, t).start()

        @pl.when(m > 0)
        def _():
            combine(m - 1)

        return 0

    lax.fori_loop(0, 4, member, 0)
    combine(3)
    base = scores[group, 0:256]

    def decode(held, first, count, at):
        whole = (base[None] + held[first : first + count].astype(F32)).reshape(32 * count, 256)
        high = whole.astype(BF16)
        low = (whole - high.astype(F32)).astype(BF16)
        both = dot(jnp.concatenate([high, low], axis=0), wide[0], 1, 0)
        value = both[: 32 * count] + both[32 * count :] + dot(high, wide[1], 1, 0)
        fields[at : at + count] = value.astype(BF16).astype(F32).reshape(count, 32, 1024)

    def arrived(m):
        remote(theirs.at[m], theirs.at[m], fs.at[m], fr.at[m], at_y(me, 4)).wait_recv()

    def gap(d):
        q = d * d + SMOOTH2
        r = lax.rsqrt(q)
        return d * r, q * r

    decode(mine, 0, 4, 0)
    for m in range(3):
        arrived(m)
    decode(theirs, 0, 3, 4)

    def early(i, _):
        cols = pl.ds(pl.multiple_of(128 * i, 128), 128)
        y = tall[group, cols]
        f = [fields[m, :, cols] for m in range(7)]
        slope = [jnp.zeros((32, 128), F32) for _ in range(4)]
        spread = jnp.zeros((32, 128), F32)
        skill = jnp.zeros((32, 128), F32)
        for m in range(7):
            for n in range(m + 1, 7):
                s, value = gap(f[m] - f[n])
                spread = spread + value
                if m < 4:
                    slope[m] = slope[m] + s
                if n < 4:
                    slope[n] = slope[n] - s
        for m in range(7):
            s, value = gap(f[m] - y)
            skill = skill + value
            if m < 4:
                slopes[m, :, cols] = s - slope[m] * (1.0 / 7.0)
        scores[0:32, cols] = skill * (1.0 / 8.0) - spread * (2.0 / 112.0)
        return 0

    lax.fori_loop(0, 8, early, 0)
    valid = lax.broadcasted_iota(jnp.int32, (32, 128), 0) + 32 * x < 100
    arrived(3)
    decode(theirs, 3, 1, 7)

    def late(i, carry):
        cols = pl.ds(pl.multiple_of(128 * i, 128), 128)
        a = area[:, cols]
        last = fields[7, :, cols]
        spread = jnp.zeros((32, 128), F32)
        for m in range(7):
            s, value = gap(fields[m, :, cols] - last)
            spread = spread + value
            if m < 4:
                made[m, :, cols] = (a * (slopes[m, :, cols] - s * (1.0 / 7.0))).astype(BF16)
        _, value = gap(last - tall[group, cols])
        score = a * (scores[0:32, cols] + value * (1.0 / 8.0) - spread * (2.0 / 112.0))
        return carry + jnp.where(valid, score, 0.0)

    total = lax.fori_loop(0, 8, late, jnp.zeros((32, 128), F32))
    l0[...] = jnp.sum(total, axis=0, keepdims=True)

    for t, spot in enumerate(spots):
        go(remote(l0, b1.at[t], ls.at[t], lr.at[t], near(*spot)))
    for t in (1, 2, 3):
        peer = at_x(me, t)
        go(remote(made.at[peer[1]], grad.at[group], gs.at[t], gr.at[t], peer))
    keep = pltpu.make_async_copy(made.at[x], grad.at[group], gs.at[0])
    keep.start()
    for t, (dx, dc, dy) in enumerate(spots):
        remote(b1.at[t], b1.at[t], ls.at[t], lr.at[t], near(-dx, dc, -dy)).wait_recv()
    l1[...] = l0[...] + jnp.sum(b1[...], axis=0)
    for t in range(7):
        go(remote(l1, b2.at[t], zs2.at[t], zr2.at[t], at_z(me, t + 1)))
    for t in range(7):
        remote(b2.at[t], b2.at[t], zs2.at[t], zr2.at[t], at_z(me, -t - 1)).wait_recv()
    value = l1[...] + jnp.sum(b2[...], axis=0)
    loss[...] = jnp.sum(value, axis=1, keepdims=True) * (1.0 / 6553600.0)
    keep.wait()
    for t in (1, 2, 3):
        peer = at_x(me, -t)
        there = pl.ds(pl.multiple_of(32 * peer[1], 32), 32)
        remote(grad.at[there], grad.at[there], gs.at[t], gr.at[t], peer).wait_recv()
    for copy in started:
        copy.wait_send()
    for m in range(4):
        for t in (1, 2, 3):
            to_x(m, t).wait_send()
        to_other(m).wait_send()


def dma(*shape):
    return pltpu.SemaphoreType.DMA(shape)


def per_device(
    node_states, noise, norm_gain, cond_weight, w_query, w_key, w_value, w_out,
    edge_src, send_rows, dec_src, dec_weight, w_decode, truth, area,
):
    grad, loss = pl.pallas_call(
        step_kernel,
        out_shape=(
            jax.ShapeDtypeStruct((128, 1024), BF16),
            jax.ShapeDtypeStruct((1, 1), F32),
        ),
        in_specs=[pl.BlockSpec(memory_space=pl.ANY)] * 15,
        out_specs=(pl.BlockSpec(memory_space=pl.ANY), VMEM),
        scratch_shapes=[
            pltpu.VMEM((256, 1024), BF16),
            pltpu.VMEM((16, 256), BF16),
            pltpu.VMEM((1, 256), jnp.int32),
            pltpu.VMEM((1, 1024), F32),
            pltpu.VMEM((16, 2048), BF16),
            pltpu.VMEM((8, 256), jnp.int32),
            pltpu.VMEM((100, 1024), BF16),
            pltpu.VMEM((3, 1024), jnp.int32),
            pltpu.VMEM((3, 1024), F32),
            pltpu.VMEM((100, 1024), BF16),
            pltpu.VMEM((1, 1024), F32),
            pltpu.VMEM((16, 1024), BF16),
            pltpu.VMEM((8, 4, 2, 16, 896), BF16),
            pltpu.VMEM((2, 128, 1024), BF16),
            pltpu.VMEM((4, 2, 16, 128), BF16),
            pltpu.VMEM((4, 16, 256), BF16),
            pltpu.VMEM((2, 128, 1024), BF16),
            pltpu.VMEM((2, 16, 128), BF16),
            pltpu.VMEM((512, 1024), F32),
            pltpu.VMEM((512, 256), F32),
            pltpu.VMEM((4, 512, 1024), BF16),
            pltpu.VMEM((256, 1024), BF16),
            pltpu.VMEM((128, 256), BF16),
            pltpu.VMEM((256, 256), BF16),
            pltpu.VMEM((4, 128, 256), BF16),
            pltpu.VMEM((4, 4, 32, 256), BF16),
            pltpu.VMEM((4, 32, 256), BF16),
            pltpu.VMEM((4, 32, 256), BF16),
            pltpu.VMEM((2, 256, 1024), BF16),
            pltpu.VMEM((128, 1024), F32),
            pltpu.VMEM((8, 32, 1024), F32),
            pltpu.VMEM((4, 32, 1024), F32),
            pltpu.VMEM((128, 1024), F32),
            pltpu.VMEM((4, 32, 1024), BF16),
            pltpu.VMEM((1, 128), F32),
            pltpu.VMEM((1, 128), F32),
            pltpu.VMEM((31, 1, 128), F32),
            pltpu.VMEM((7, 1, 128), F32),
            dma(16),
            dma(8), dma(8), dma(8, 3), dma(8, 3), dma(8), dma(8), dma(2), dma(2), dma(2), dma(2),
            dma(4, 3), dma(4, 3), dma(4, 4), dma(4, 4), dma(4), dma(4), dma(4), dma(4),
            dma(31), dma(31), dma(7), dma(7),
        ],
        compiler_params=pltpu.CompilerParams(collective_id=0, has_side_effects=True),
        name="step",
    )(
        w_query, w_key, w_value, w_out, node_states, noise[0], send_rows.reshape(1, 256),
        norm_gain.reshape(1, 1024), cond_weight, edge_src, w_decode,
        dec_src, dec_weight, truth, area.reshape(1, 1024),
    )
    return loss[0, 0], grad[None, :100]


def solution(mesh):
    split = Mesh(mesh.devices.reshape(2, 4, 8, 4, 2), MEMBER + SPACE)
    return jax.shard_map(
        per_device,
        mesh=split,
        in_specs=(
            P(SPACE, None),
            P(MEMBER, None, SPACE),
            P(),
            P(),
            P(SPACE, None),
            P(SPACE, None),
            P(SPACE, None),
            P(SPACE, None),
            P(None, SPACE),
            P(SPACE),
            P(None, SPACE),
            P(None, SPACE),
            P(),
            P(None, SPACE),
            P(SPACE),
        ),
        out_specs=(P(), P(MEMBER, None, SPACE)),
        check_vma=False,
    )
```

```python
import functools

import jax
import jax.numpy as jnp
from jax import lax
from jax.experimental import pallas as pl
from jax.experimental.pallas import tpu as pltpu
from jax.sharding import Mesh
from jax.sharding import PartitionSpec as P

SPACE = ("space_0", "space_1", "space_2")
MEMBER = ("member_0", "member_1")
SMOOTH2 = 0.0625
EPS = 1e-05
F32 = jnp.float32
BF16 = jnp.bfloat16
NEG = -1e30
LARGEST = jnp.finfo(jnp.bfloat16).max
VMEM = pl.BlockSpec(memory_space=pltpu.VMEM)

OFFSETS = (1, 7, 2, 6, 3, 5, 4)


def dot(a, b, ca, cb):
    return lax.dot_general(a, b, (((ca,), (cb,)), ((), ())), preferred_element_type=F32)


def place():
    return tuple(lax.axis_index(a) for a in MEMBER + SPACE)


def remote(src, dst, send, recv, device):
    return pltpu.make_async_remote_copy(
        src_ref=src,
        dst_ref=dst,
        send_sem=send,
        recv_sem=recv,
        device_id=device,
        device_id_type=pl.DeviceIdType.MESH,
    )


def at_y(me, step):
    yh, x, z, yl, c = me
    y = lax.rem(4 * yh + yl + 8 + step, 8)
    return (y // 4, x, z, lax.rem(y, 4), c)


def at_z(me, step):
    yh, x, z, yl, c = me
    return (yh, x, lax.rem(z + 8 + step, 8), yl, c)


def at_x(me, step):
    yh, x, z, yl, c = me
    return (yh, lax.rem(x + 4 + step, 4), z, yl, c)


def at_core(me):
    yh, x, z, yl, c = me
    return (yh, x, z, yl, 1 - c)


def at_block(me, step):
    yh, x, z, yl, c = me
    s = lax.rem(z * 8 + yl * 2 + c + 64 + step, 64)
    return (yh, x, s // 8, lax.rem(s, 8) // 2, lax.rem(s, 2))


def greet(devices):
    barrier = pltpu.get_barrier_semaphore()
    for d in devices:
        pl.semaphore_signal(barrier, inc=1, device_id=d, device_id_type=pl.DeviceIdType.MESH)
    return lambda: pl.semaphore_wait(barrier, len(devices))


def step_kernel(
    wq, wk, wv, wo, states_in, noise_in, rows_in, gain_in, cond_in, edges_in, wd_in,
    source_in, weight_in, truth_in, area_in,
    grad, loss,
    states, noise, rows, gain, cond, edges, wd, source, weight, truth, area, wo_here,
    wall, halo, nhalo, nown, picked, npicked,
    normed, counts, hidden, wvt, w2t, att,
    part, got, mine, theirs, wide, tall, fields, slopes, scores, made, l0, l1, b1, b2,
    fetch, zs, zr, ys, yr, cs, cr, hs, hr, ns, nr, xs, xr, ps, pr, fs, fr, gs, gr, ls, lr, zs2, zr2,
):
    me = place()
    yh, x, z, yl, c = me
    spots = [(dx, dc, dy) for dy in (2, 1, -1, 0) for dx in range(4) for dc in range(2) if dx or dc or dy]

    def near(dx, dc, dy):
        yh_, _, _, yl_, _ = at_y(me, dy)
        return (yh_, lax.rem(x + 4 + dx, 4), z, yl_, lax.rem(c + dc, 2))

    wait_all = greet(
        [at_z(me, o) for o in OFFSETS]
        + [at_y(me, o) for o in (1, -1, 2, -2, 4)]
        + [at_core(me)]
        + [at_x(me, o) for o in (1, 2, 3)]
        + [at_block(me, 1), at_block(me, -1)]
        + [near(-dx, dc, -dy) for dx, dc, dy in spots]
    )
    columns = pl.ds(pl.multiple_of(256 * x, 256), 256)
    own = wall.at[z, yl, c]
    fetches = [
        pltpu.make_async_copy(a, b, fetch.at[i])
        for i, (a, b) in enumerate(
            (
                (rows_in, rows),
                (states_in, states),
                (noise_in, noise),
                (noise_in, nown.at[x]),
                (wo, wo_here),
                (wd_in, wd),
                (wq.at[:, columns], own.at[:, 0:256]),
                (wk.at[:, columns], own.at[:, 256:512]),
                (wv.at[:, columns], own.at[:, 512:768]),
                (gain_in, gain),
                (cond_in, cond),
                (edges_in, edges),
                (source_in, source),
                (weight_in, weight),
                (truth_in, truth),
                (area_in, area),
            )
        )
    ]
    for f in fetches:
        f.start()
    for f in fetches[:3]:
        f.wait()
    chosen = (lax.broadcasted_iota(jnp.int32, (256, 256), 0) == rows[...]).astype(F32).astype(BF16)
    picked[...] = dot(chosen, states[...], 0, 0).astype(BF16).reshape(2, 128, 1024)
    sent_noise = dot(noise[...], chosen, 1, 0).astype(BF16)
    npicked[0] = sent_noise[:, 0:128]
    npicked[1] = sent_noise[:, 128:256]
    for f in fetches[3:9]:
        f.wait()
    wall[z, yl, c, :, 768:868] = dot(wo_here[...], wd[...], 1, 1).astype(BF16)
    wall[z, yl, c, :, 868:896] = jnp.zeros((16, 28), BF16)
    wait_all()

    started = []

    def go(copy):
        copy.start()
        started.append(copy)

    quarter = pl.ds(pl.multiple_of(32 * x, 32), 32)
    for i, (half, step) in enumerate(((1, 1), (0, -1))):
        go(remote(picked.at[half, quarter], halo.at[i, quarter], hs.at[i], hr.at[i], at_block(me, step)))
        go(remote(npicked.at[half], nhalo.at[x, i], ns.at[i], nr.at[i], at_block(me, step)))
    for o in OFFSETS:
        go(remote(own, own, zs.at[o], zr.at[o], at_z(me, o)))
    for t in (1, 2, 3):
        go(remote(nown.at[x], nown.at[x], xs.at[t, 0], xr.at[t, 0], at_x(me, t)))

    def y_steps(k):
        return (1, -1, 2 if k % 2 == 0 else -2)

    order = (0,) + OFFSETS

    def forward_y(k):
        zk = lax.rem(z + 8 - order[k], 8)
        block = wall.at[zk, yl, c]
        if k:
            remote(block, block, zs.at[order[k]], zr.at[order[k]], at_z(me, -order[k])).wait_recv()
        for t, step in enumerate(y_steps(k)):
            go(remote(block, block, ys.at[k, t], yr.at[k, t], at_y(me, step)))

    def forward_core(k):
        zk = lax.rem(z + 8 - order[k], 8)
        for t, step in enumerate(y_steps(k)):
            landed = wall.at[zk, lax.rem(yl + 4 - step, 4), c]
            remote(landed, landed, ys.at[k, t], yr.at[k, t], at_y(me, -step)).wait_recv()
        both = wall.at[zk, :, c]
        go(remote(both, both, cs.at[k], cr.at[k], at_core(me)))

    def forward_x():
        for i, step in enumerate((1, -1)):
            slot = halo.at[i, quarter]
            remote(slot, slot, hs.at[i], hr.at[i], at_block(me, -step)).wait_recv()
            slot = nhalo.at[x, i]
            remote(slot, slot, ns.at[i], nr.at[i], at_block(me, -step)).wait_recv()
        for t in (1, 2, 3):
            go(remote(halo.at[:, quarter], halo.at[:, quarter], xs.at[t, 1], xr.at[t, 1], at_x(me, t)))
            go(remote(nhalo.at[x], nhalo.at[x], xs.at[t, 2], xr.at[t, 2], at_x(me, t)))

    def normalise(values, at):
        v = values.astype(F32)
        center = v - jnp.mean(v, axis=1, keepdims=True)
        spread = jnp.mean(center * center, axis=1, keepdims=True)
        normed[at : at + 128, :] = center * lax.rsqrt(spread + EPS) * gain[...]

    def condition(i, noises):
        rows = slice(128 * i, 128 * i + 128)
        for m in range(4):
            terms = dot(noises(m), cond[...], 0, 0)
            hidden[m, rows, :] = (normed[rows, :] * (1.0 + terms[:, :1024]) + terms[:, 1024:]).astype(BF16)

    forward_y(0)
    for f in fetches[9:]:
        f.wait()
    normalise(states[0:128, :], 128)
    forward_y(1)
    forward_y(2)
    normalise(states[128:256, :], 256)
    forward_y(3)
    forward_y(4)
    forward_x()
    row = lax.broadcasted_iota(jnp.int32, (512, 256), 0)
    total = jnp.zeros((512, 256), F32)
    for k in range(8):
        total = total + (row == edges[k : k + 1, :]).astype(F32)
    counts[...] = jnp.where(total > 0.0, jnp.log(jnp.maximum(total, 1.0)), NEG).T
    forward_y(5)
    forward_y(6)
    forward_y(7)
    forward_core(0)
    forward_core(1)
    for t in (1, 2, 3):
        other = lax.rem(x + 4 - t, 4)
        slot = nown.at[other]
        remote(slot, slot, xs.at[t, 0], xr.at[t, 0], at_x(me, -t)).wait_recv()
    condition(1, lambda m: nown[m, :, 0:128])
    forward_core(2)
    condition(2, lambda m: nown[m, :, 128:256])
    forward_core(3)
    for t in (1, 2, 3):
        other = lax.rem(x + 4 - t, 4)
        slot = halo.at[:, pl.ds(pl.multiple_of(32 * other, 32), 32)]
        remote(slot, slot, xs.at[t, 1], xr.at[t, 1], at_x(me, -t)).wait_recv()
        slot = nhalo.at[other]
        remote(slot, slot, xs.at[t, 2], xr.at[t, 2], at_x(me, -t)).wait_recv()
    normalise(halo[0], 0)
    condition(0, lambda m: nhalo[m, 0])
    forward_core(4)
    normalise(halo[1], 384)
    condition(3, lambda m: nhalo[m, 1])
    forward_core(5)
    node = lax.broadcasted_iota(jnp.int32, (256, 1024), 0)
    select = jnp.zeros((256, 1024), F32)
    for k in range(3):
        select = select + jnp.where(node == source[k : k + 1, :], weight[k : k + 1, :], 0.0)
    wide[0] = select.astype(BF16)
    wide[1] = (select - wide[0].astype(F32)).astype(BF16)
    forward_core(6)
    tall[0:100, :] = truth[...].astype(F32)
    tall[100:128, :] = jnp.zeros((28, 1024), F32)
    base = dot(wd[...], states[...], 1, 1)
    scores[0:100, 0:256] = base
    scores[100:128, 0:256] = jnp.zeros((28, 256), F32)
    forward_core(7)
    for k, o in enumerate(order):
        landed = wall.at[lax.rem(z + 8 - o, 8), :, 1 - c]
        remote(landed, landed, cs.at[k], cr.at[k], at_core(me)).wait_recv()

    w2t[...] = wall[pl.ds(2 * x, 2)].reshape(256, 896)[:, 768:896].T
    lane = lax.broadcasted_iota(jnp.int32, (256, 256), 1) // 64
    group = quarter

    def to_x(m, t):
        peer = at_x(me, t)
        there = pl.ds(pl.multiple_of(32 * peer[1], 32), 32)
        return remote(part.at[m, there], got.at[m, t], ps.at[m, t], pr.at[m, t], peer)

    def to_other(m):
        return remote(mine.at[m], theirs.at[m], fs.at[m], fr.at[m], at_y(me, 4))

    def combine(m):
        update = part[m, group, :].astype(F32)
        for t in (1, 2, 3):
            remote(got.at[m, t], got.at[m, t], ps.at[m, t], pr.at[m, t], at_x(me, -t)).wait_recv()
            update = update + got[m, t].astype(F32)
        mine[m] = update.astype(BF16)
        to_other(m).start()

    def member(m, _):
        all_rows = hidden[m]
        w = wall[...].reshape(1024, 896)
        query = dot(hidden[m, 128:384, :], w[:, 0:256], 1, 0).astype(BF16) * 0.125
        key = dot(all_rows, w[:, 256:512], 1, 0).astype(BF16)
        value = dot(all_rows, w[:, 512:768], 1, 0).astype(BF16)
        for h in range(4):
            one = jnp.where(lane == h, query, jnp.zeros_like(query))
            share = jnp.exp(dot(one, key, 1, 1) + counts[...])
            below = jnp.sum(share, axis=1, keepdims=True)
            rounded = jnp.minimum(share.astype(BF16), LARGEST)
            above = dot(rounded, value, 1, 0) / below
            if h:
                above = jnp.where(lane == h, above, att[...])
            att[...] = above
        part[m] = dot(w2t[...], att[...].astype(BF16), 1, 1).astype(BF16)
        for t in (1, 2, 3):
            to_x(m, t).start()

        @pl.when(m > 0)
        def _():
            combine(m - 1)

        return 0

    lax.fori_loop(0, 4, member, 0)
    combine(3)
    base = scores[group, 0:256]

    def decode(held, first, count, at):
        whole = (base[None] + held[first : first + count].astype(F32)).reshape(32 * count, 256)
        high = whole.astype(BF16)
        low = (whole - high.astype(F32)).astype(BF16)
        both = dot(jnp.concatenate([high, low], axis=0), wide[0], 1, 0)
        value = both[: 32 * count] + both[32 * count :] + dot(high, wide[1], 1, 0)
        fields[at : at + count] = value.astype(BF16).astype(F32).reshape(count, 32, 1024)

    def arrived(m):
        remote(theirs.at[m], theirs.at[m], fs.at[m], fr.at[m], at_y(me, 4)).wait_recv()

    def gap(d):
        q = d * d + SMOOTH2
        r = lax.rsqrt(q)
        return d * r, q * r

    decode(mine, 0, 4, 0)
    for m in range(3):
        arrived(m)
    decode(theirs, 0, 3, 4)

    def early(i, _):
        cols = pl.ds(pl.multiple_of(128 * i, 128), 128)
        y = tall[group, cols]
        f = [fields[m, :, cols] for m in range(7)]
        slope = [jnp.zeros((32, 128), F32) for _ in range(4)]
        spread = jnp.zeros((32, 128), F32)
        skill = jnp.zeros((32, 128), F32)
        for m in range(7):
            for n in range(m + 1, 7):
                s, value = gap(f[m] - f[n])
                spread = spread + value
                if m < 4:
                    slope[m] = slope[m] + s
                if n < 4:
                    slope[n] = slope[n] - s
        for m in range(7):
            s, value = gap(f[m] - y)
            skill = skill + value
            if m < 4:
                slopes[m, :, cols] = s - slope[m] * (1.0 / 7.0)
        scores[0:32, cols] = skill * (1.0 / 8.0) - spread * (2.0 / 112.0)
        return 0

    lax.fori_loop(0, 8, early, 0)
    valid = lax.broadcasted_iota(jnp.int32, (32, 128), 0) + 32 * x < 100
    arrived(3)
    decode(theirs, 3, 1, 7)

    def late(i, carry):
        cols = pl.ds(pl.multiple_of(128 * i, 128), 128)
        a = area[:, cols]
        last = fields[7, :, cols]
        spread = jnp.zeros((32, 128), F32)
        for m in range(7):
            s, value = gap(fields[m, :, cols] - last)
            spread = spread + value
            if m < 4:
                made[m, :, cols] = (a * (slopes[m, :, cols] - s * (1.0 / 7.0))).astype(BF16)
        _, value = gap(last - tall[group, cols])
        score = a * (scores[0:32, cols] + value * (1.0 / 8.0) - spread * (2.0 / 112.0))
        return carry + jnp.where(valid, score, 0.0)

    total = lax.fori_loop(0, 8, late, jnp.zeros((32, 128), F32))
    l0[...] = jnp.sum(total, axis=0, keepdims=True)

    for t, spot in enumerate(spots):
        go(remote(l0, b1.at[t], ls.at[t], lr.at[t], near(*spot)))
    for t in (1, 2, 3):
        peer = at_x(me, t)
        go(remote(made.at[peer[1]], grad.at[group], gs.at[t], gr.at[t], peer))
    keep = pltpu.make_async_copy(made.at[x], grad.at[group], gs.at[0])
    keep.start()
    for t, (dx, dc, dy) in enumerate(spots):
        remote(b1.at[t], b1.at[t], ls.at[t], lr.at[t], near(-dx, dc, -dy)).wait_recv()
    l1[...] = l0[...] + jnp.sum(b1[...], axis=0)
    for t in range(7):
        go(remote(l1, b2.at[t], zs2.at[t], zr2.at[t], at_z(me, t + 1)))
    for t in range(7):
        remote(b2.at[t], b2.at[t], zs2.at[t], zr2.at[t], at_z(me, -t - 1)).wait_recv()
    value = l1[...] + jnp.sum(b2[...], axis=0)
    loss[...] = jnp.sum(value, axis=1, keepdims=True) * (1.0 / 6553600.0)
    keep.wait()
    for t in (1, 2, 3):
        peer = at_x(me, -t)
        there = pl.ds(pl.multiple_of(32 * peer[1], 32), 32)
        remote(grad.at[there], grad.at[there], gs.at[t], gr.at[t], peer).wait_recv()
    for copy in started:
        copy.wait_send()
    for m in range(4):
        for t in (1, 2, 3):
            to_x(m, t).wait_send()
        to_other(m).wait_send()


def dma(*shape):
    return pltpu.SemaphoreType.DMA(shape)


def per_device(
    node_states, noise, norm_gain, cond_weight, w_query, w_key, w_value, w_out,
    edge_src, send_rows, dec_src, dec_weight, w_decode, truth, area,
):
    grad, loss = pl.pallas_call(
        step_kernel,
        out_shape=(
            jax.ShapeDtypeStruct((128, 1024), BF16),
            jax.ShapeDtypeStruct((1, 1), F32),
        ),
        in_specs=[pl.BlockSpec(memory_space=pl.ANY)] * 15,
        out_specs=(pl.BlockSpec(memory_space=pl.ANY), VMEM),
        scratch_shapes=[
            pltpu.VMEM((256, 1024), BF16),
            pltpu.VMEM((16, 256), BF16),
            pltpu.VMEM((1, 256), jnp.int32),
            pltpu.VMEM((1, 1024), F32),
            pltpu.VMEM((16, 2048), BF16),
            pltpu.VMEM((8, 256), jnp.int32),
            pltpu.VMEM((100, 1024), BF16),
            pltpu.VMEM((3, 1024), jnp.int32),
            pltpu.VMEM((3, 1024), F32),
            pltpu.VMEM((100, 1024), BF16),
            pltpu.VMEM((1, 1024), F32),
            pltpu.VMEM((16, 1024), BF16),
            pltpu.VMEM((8, 4, 2, 16, 896), BF16),
            pltpu.VMEM((2, 128, 1024), BF16),
            pltpu.VMEM((4, 2, 16, 128), BF16),
            pltpu.VMEM((4, 16, 256), BF16),
            pltpu.VMEM((2, 128, 1024), BF16),
            pltpu.VMEM((2, 16, 128), BF16),
            pltpu.VMEM((512, 1024), F32),
            pltpu.VMEM((256, 512), F32),
            pltpu.VMEM((4, 512, 1024), BF16),
            pltpu.VMEM((16, 128), BF16),
            pltpu.VMEM((128, 256), BF16),
            pltpu.VMEM((256, 256), F32),
            pltpu.VMEM((4, 128, 256), BF16),
            pltpu.VMEM((4, 4, 32, 256), BF16),
            pltpu.VMEM((4, 32, 256), BF16),
            pltpu.VMEM((4, 32, 256), BF16),
            pltpu.VMEM((2, 256, 1024), BF16),
            pltpu.VMEM((128, 1024), F32),
            pltpu.VMEM((8, 32, 1024), F32),
            pltpu.VMEM((4, 32, 1024), F32),
            pltpu.VMEM((128, 1024), F32),
            pltpu.VMEM((4, 32, 1024), BF16),
            pltpu.VMEM((1, 128), F32),
            pltpu.VMEM((1, 128), F32),
            pltpu.VMEM((31, 1, 128), F32),
            pltpu.VMEM((7, 1, 128), F32),
            dma(16),
            dma(8), dma(8), dma(8, 3), dma(8, 3), dma(8), dma(8), dma(2), dma(2), dma(2), dma(2),
            dma(4, 3), dma(4, 3), dma(4, 4), dma(4, 4), dma(4), dma(4), dma(4), dma(4),
            dma(31), dma(31), dma(7), dma(7),
        ],
        compiler_params=pltpu.CompilerParams(collective_id=0, has_side_effects=True),
        name="step",
    )(
        w_query, w_key, w_value, w_out, node_states, noise[0], send_rows.reshape(1, 256),
        norm_gain.reshape(1, 1024), cond_weight, edge_src, w_decode,
        dec_src, dec_weight, truth, area.reshape(1, 1024),
    )
    return loss[0, 0], grad[None, :100]


def solution(mesh):
    split = Mesh(mesh.devices.reshape(2, 4, 8, 4, 2), MEMBER + SPACE)
    return jax.shard_map(
        per_device,
        mesh=split,
        in_specs=(
            P(SPACE, None),
            P(MEMBER, None, SPACE),
            P(),
            P(),
            P(SPACE, None),
            P(SPACE, None),
            P(SPACE, None),
            P(SPACE, None),
            P(None, SPACE),
            P(SPACE),
            P(None, SPACE),
            P(None, SPACE),
            P(),
            P(None, SPACE),
            P(SPACE),
        ),
        out_specs=(P(), P(MEMBER, None, SPACE)),
        check_vma=False,
    )
```

```python
import functools

import jax
import jax.numpy as jnp
from jax import lax
from jax.experimental import pallas as pl
from jax.experimental.pallas import tpu as pltpu
from jax.sharding import Mesh
from jax.sharding import PartitionSpec as P

SPACE = ("space_0", "space_1", "space_2")
MEMBER = ("member_0", "member_1")
SMOOTH2 = 0.0625
EPS = 1e-05
F32 = jnp.float32
BF16 = jnp.bfloat16
NEG = -1e30
SCALE = 0.125 * 1.4426950408889634
LARGEST = jnp.finfo(jnp.bfloat16).max
VMEM = pl.BlockSpec(memory_space=pltpu.VMEM)

OFFSETS = (1, 7, 2, 6, 3, 5, 4)


def dot(a, b, ca, cb):
    return lax.dot_general(a, b, (((ca,), (cb,)), ((), ())), preferred_element_type=F32)


def place():
    return tuple(lax.axis_index(a) for a in MEMBER + SPACE)


def remote(src, dst, send, recv, device):
    return pltpu.make_async_remote_copy(
        src_ref=src,
        dst_ref=dst,
        send_sem=send,
        recv_sem=recv,
        device_id=device,
        device_id_type=pl.DeviceIdType.MESH,
    )


def at_y(me, step):
    yh, x, z, yl, c = me
    y = lax.rem(4 * yh + yl + 8 + step, 8)
    return (y // 4, x, z, lax.rem(y, 4), c)


def at_z(me, step):
    yh, x, z, yl, c = me
    return (yh, x, lax.rem(z + 8 + step, 8), yl, c)


def at_x(me, step):
    yh, x, z, yl, c = me
    return (yh, lax.rem(x + 4 + step, 4), z, yl, c)


def at_core(me):
    yh, x, z, yl, c = me
    return (yh, x, z, yl, 1 - c)


def at_block(me, step):
    yh, x, z, yl, c = me
    s = lax.rem(z * 8 + yl * 2 + c + 64 + step, 64)
    return (yh, x, s // 8, lax.rem(s, 8) // 2, lax.rem(s, 2))


def greet(devices):
    barrier = pltpu.get_barrier_semaphore()
    for d in devices:
        pl.semaphore_signal(barrier, inc=1, device_id=d, device_id_type=pl.DeviceIdType.MESH)
    return lambda: pl.semaphore_wait(barrier, len(devices))


def step_kernel(
    wq, wk, wv, wo, states_in, noise_in, rows_in, gain_in, cond_in, edges_in, wd_in,
    source_in, weight_in, truth_in, area_in,
    grad, loss,
    states, noise, rows, gain, cond, edges, wd, source, weight, truth, area, wo_here,
    wall, halo, nhalo, nown, picked, npicked,
    normed, counts, hidden, wvt, w2t, att,
    part, got, mine, theirs, wide, tall, fields, slopes, scores, made, l0, l1, b1, b2,
    fetch, zs, zr, ys, yr, cs, cr, hs, hr, ns, nr, xs, xr, ps, pr, fs, fr, gs, gr, ls, lr, zs2, zr2,
):
    me = place()
    yh, x, z, yl, c = me
    spots = [(dx, dc, dy) for dy in (2, 1, -1, 0) for dx in range(4) for dc in range(2) if dx or dc or dy]

    def near(dx, dc, dy):
        yh_, _, _, yl_, _ = at_y(me, dy)
        return (yh_, lax.rem(x + 4 + dx, 4), z, yl_, lax.rem(c + dc, 2))

    wait_all = greet(
        [at_z(me, o) for o in OFFSETS]
        + [at_y(me, o) for o in (1, -1, 2, -2, 4)]
        + [at_core(me)]
        + [at_x(me, o) for o in (1, 2, 3)]
        + [at_block(me, 1), at_block(me, -1)]
        + [near(-dx, dc, -dy) for dx, dc, dy in spots]
    )
    columns = pl.ds(pl.multiple_of(256 * x, 256), 256)
    own = wall.at[z, yl, c]
    fetches = [
        pltpu.make_async_copy(a, b, fetch.at[i])
        for i, (a, b) in enumerate(
            (
                (rows_in, rows),
                (states_in, states),
                (noise_in, noise),
                (noise_in, nown.at[x]),
                (wo, wo_here),
                (wd_in, wd),
                (wq.at[:, columns], own.at[:, 0:256]),
                (wk.at[:, columns], own.at[:, 256:512]),
                (wv.at[:, columns], own.at[:, 512:768]),
                (gain_in, gain),
                (cond_in, cond),
                (edges_in, edges),
                (source_in, source),
                (weight_in, weight),
                (truth_in, truth),
                (area_in, area),
            )
        )
    ]
    for f in fetches:
        f.start()
    for f in fetches[:3]:
        f.wait()
    chosen = (lax.broadcasted_iota(jnp.int32, (256, 256), 0) == rows[...]).astype(F32).astype(BF16)
    picked[...] = dot(chosen, states[...], 0, 0).astype(BF16).reshape(2, 128, 1024)
    sent_noise = dot(noise[...], chosen, 1, 0).astype(BF16)
    npicked[0] = sent_noise[:, 0:128]
    npicked[1] = sent_noise[:, 128:256]
    for f in fetches[3:9]:
        f.wait()
    wall[z, yl, c, :, 768:868] = dot(wo_here[...], wd[...], 1, 1).astype(BF16)
    wall[z, yl, c, :, 868:896] = jnp.zeros((16, 28), BF16)
    wait_all()

    started = []

    def go(copy):
        copy.start()
        started.append(copy)

    quarter = pl.ds(pl.multiple_of(32 * x, 32), 32)
    for i, (half, step) in enumerate(((1, 1), (0, -1))):
        go(remote(picked.at[half, quarter], halo.at[i, quarter], hs.at[i], hr.at[i], at_block(me, step)))
        go(remote(npicked.at[half], nhalo.at[x, i], ns.at[i], nr.at[i], at_block(me, step)))
    for o in OFFSETS:
        go(remote(own, own, zs.at[o], zr.at[o], at_z(me, o)))
    for t in (1, 2, 3):
        go(remote(nown.at[x], nown.at[x], xs.at[t, 0], xr.at[t, 0], at_x(me, t)))

    def y_steps(k):
        return (1, -1, 2 if k % 2 == 0 else -2)

    order = (0,) + OFFSETS

    def forward_y(k):
        zk = lax.rem(z + 8 - order[k], 8)
        block = wall.at[zk, yl, c]
        if k:
            remote(block, block, zs.at[order[k]], zr.at[order[k]], at_z(me, -order[k])).wait_recv()
        for t, step in enumerate(y_steps(k)):
            go(remote(block, block, ys.at[k, t], yr.at[k, t], at_y(me, step)))

    def forward_core(k):
        zk = lax.rem(z + 8 - order[k], 8)
        for t, step in enumerate(y_steps(k)):
            landed = wall.at[zk, lax.rem(yl + 4 - step, 4), c]
            remote(landed, landed, ys.at[k, t], yr.at[k, t], at_y(me, -step)).wait_recv()
        both = wall.at[zk, :, c]
        go(remote(both, both, cs.at[k], cr.at[k], at_core(me)))

    def forward_x():
        for i, step in enumerate((1, -1)):
            slot = halo.at[i, quarter]
            remote(slot, slot, hs.at[i], hr.at[i], at_block(me, -step)).wait_recv()
            slot = nhalo.at[x, i]
            remote(slot, slot, ns.at[i], nr.at[i], at_block(me, -step)).wait_recv()
        for t in (1, 2, 3):
            go(remote(halo.at[:, quarter], halo.at[:, quarter], xs.at[t, 1], xr.at[t, 1], at_x(me, t)))
            go(remote(nhalo.at[x], nhalo.at[x], xs.at[t, 2], xr.at[t, 2], at_x(me, t)))

    def normalise(values, at):
        v = values.astype(F32)
        center = v - jnp.mean(v, axis=1, keepdims=True)
        spread = jnp.mean(center * center, axis=1, keepdims=True)
        normed[at : at + 128, :] = center * lax.rsqrt(spread + EPS) * gain[...]

    def condition(i, noises):
        rows = slice(128 * i, 128 * i + 128)
        for m in range(4):
            terms = dot(noises(m), cond[...], 0, 0)
            hidden[m, rows, :] = (normed[rows, :] * (1.0 + terms[:, :1024]) + terms[:, 1024:]).astype(BF16)

    forward_y(0)
    for f in fetches[9:]:
        f.wait()
    normalise(states[0:128, :], 128)
    forward_y(1)
    forward_y(2)
    normalise(states[128:256, :], 256)
    forward_y(3)
    forward_y(4)
    forward_x()
    row = lax.broadcasted_iota(jnp.int32, (512, 256), 0)
    total = jnp.zeros((512, 256), F32)
    for k in range(8):
        total = total + (row == edges[k : k + 1, :]).astype(F32)
    counts[...] = jnp.where(total > 0.0, jnp.log2(jnp.maximum(total, 1.0)), NEG).T
    forward_y(5)
    forward_y(6)
    forward_y(7)
    forward_core(0)
    forward_core(1)
    for t in (1, 2, 3):
        other = lax.rem(x + 4 - t, 4)
        slot = nown.at[other]
        remote(slot, slot, xs.at[t, 0], xr.at[t, 0], at_x(me, -t)).wait_recv()
    condition(1, lambda m: nown[m, :, 0:128])
    forward_core(2)
    condition(2, lambda m: nown[m, :, 128:256])
    forward_core(3)
    for t in (1, 2, 3):
        other = lax.rem(x + 4 - t, 4)
        slot = halo.at[:, pl.ds(pl.multiple_of(32 * other, 32), 32)]
        remote(slot, slot, xs.at[t, 1], xr.at[t, 1], at_x(me, -t)).wait_recv()
        slot = nhalo.at[other]
        remote(slot, slot, xs.at[t, 2], xr.at[t, 2], at_x(me, -t)).wait_recv()
    normalise(halo[0], 0)
    condition(0, lambda m: nhalo[m, 0])
    forward_core(4)
    normalise(halo[1], 384)
    condition(3, lambda m: nhalo[m, 1])
    forward_core(5)
    node = lax.broadcasted_iota(jnp.int32, (256, 1024), 0)
    select = jnp.zeros((256, 1024), F32)
    for k in range(3):
        select = select + jnp.where(node == source[k : k + 1, :], weight[k : k + 1, :], 0.0)
    wide[0] = select.astype(BF16)
    wide[1] = (select - wide[0].astype(F32)).astype(BF16)
    forward_core(6)
    tall[0:100, :] = truth[...].astype(F32)
    tall[100:128, :] = jnp.zeros((28, 1024), F32)
    base = dot(wd[...], states[...], 1, 1)
    scores[0:100, 0:256] = base
    scores[100:128, 0:256] = jnp.zeros((28, 256), F32)
    forward_core(7)
    for k, o in enumerate(order):
        landed = wall.at[lax.rem(z + 8 - o, 8), :, 1 - c]
        remote(landed, landed, cs.at[k], cr.at[k], at_core(me)).wait_recv()

    w2t[...] = wall[pl.ds(2 * x, 2)].reshape(256, 896)[:, 768:896].T
    lane = lax.broadcasted_iota(jnp.int32, (256, 256), 1) // 64
    group = quarter

    def to_x(m, t):
        peer = at_x(me, t)
        there = pl.ds(pl.multiple_of(32 * peer[1], 32), 32)
        return remote(part.at[m, there], got.at[m, t], ps.at[m, t], pr.at[m, t], peer)

    def to_other(m):
        return remote(mine.at[m], theirs.at[m], fs.at[m], fr.at[m], at_y(me, 4))

    def combine(m):
        update = part[m, group, :].astype(F32)
        for t in (1, 2, 3):
            remote(got.at[m, t], got.at[m, t], ps.at[m, t], pr.at[m, t], at_x(me, -t)).wait_recv()
            update = update + got[m, t].astype(F32)
        mine[m] = update.astype(BF16)
        to_other(m).start()

    def member(m, _):
        all_rows = hidden[m]
        w = wall[...].reshape(1024, 896)
        query = (dot(hidden[m, 128:384, :], w[:, 0:256], 1, 0) * SCALE).astype(BF16)
        key = dot(all_rows, w[:, 256:512], 1, 0).astype(BF16)
        value = dot(all_rows, w[:, 512:768], 1, 0).astype(BF16)
        for h in range(4):
            one = jnp.where(lane == h, query, jnp.zeros_like(query))
            share = jnp.exp2(dot(one, key, 1, 1) + counts[...])
            below = jnp.sum(share, axis=1, keepdims=True)
            rounded = jnp.minimum(share.astype(BF16), LARGEST)
            above = dot(rounded, value, 1, 0) / below
            if h:
                above = jnp.where(lane == h, above, att[...])
            att[...] = above
        part[m] = dot(w2t[...], att[...].astype(BF16), 1, 1).astype(BF16)
        for t in (1, 2, 3):
            to_x(m, t).start()

        @pl.when(m > 0)
        def _():
            combine(m - 1)

        return 0

    lax.fori_loop(0, 4, member, 0)
    combine(3)
    base = scores[group, 0:256]

    def decode(held, first, count, at):
        whole = (base[None] + held[first : first + count].astype(F32)).reshape(32 * count, 256)
        high = whole.astype(BF16)
        low = (whole - high.astype(F32)).astype(BF16)
        both = dot(jnp.concatenate([high, low], axis=0), wide[0], 1, 0)
        value = both[: 32 * count] + both[32 * count :] + dot(high, wide[1], 1, 0)
        fields[at : at + count] = value.astype(BF16).astype(F32).reshape(count, 32, 1024)

    def arrived(m):
        remote(theirs.at[m], theirs.at[m], fs.at[m], fr.at[m], at_y(me, 4)).wait_recv()

    def gap(d):
        q = d * d + SMOOTH2
        r = lax.rsqrt(q)
        return d * r, q * r

    decode(mine, 0, 4, 0)
    for m in range(3):
        arrived(m)
    decode(theirs, 0, 3, 4)

    def early(i, _):
        cols = pl.ds(pl.multiple_of(128 * i, 128), 128)
        y = tall[group, cols]
        f = [fields[m, :, cols] for m in range(7)]
        slope = [jnp.zeros((32, 128), F32) for _ in range(4)]
        spread = jnp.zeros((32, 128), F32)
        skill = jnp.zeros((32, 128), F32)
        for m in range(7):
            for n in range(m + 1, 7):
                s, value = gap(f[m] - f[n])
                spread = spread + value
                if m < 4:
                    slope[m] = slope[m] + s
                if n < 4:
                    slope[n] = slope[n] - s
        for m in range(7):
            s, value = gap(f[m] - y)
            skill = skill + value
            if m < 4:
                slopes[m, :, cols] = s - slope[m] * (1.0 / 7.0)
        scores[0:32, cols] = skill * (1.0 / 8.0) - spread * (2.0 / 112.0)
        return 0

    lax.fori_loop(0, 8, early, 0)
    valid = lax.broadcasted_iota(jnp.int32, (32, 128), 0) + 32 * x < 100
    arrived(3)
    decode(theirs, 3, 1, 7)

    def late(i, carry):
        cols = pl.ds(pl.multiple_of(128 * i, 128), 128)
        a = area[:, cols]
        last = fields[7, :, cols]
        spread = jnp.zeros((32, 128), F32)
        for m in range(7):
            s, value = gap(fields[m, :, cols] - last)
            spread = spread + value
            if m < 4:
                made[m, :, cols] = (a * (slopes[m, :, cols] - s * (1.0 / 7.0))).astype(BF16)
        _, value = gap(last - tall[group, cols])
        score = a * (scores[0:32, cols] + value * (1.0 / 8.0) - spread * (2.0 / 112.0))
        return carry + jnp.where(valid, score, 0.0)

    total = lax.fori_loop(0, 8, late, jnp.zeros((32, 128), F32))
    l0[...] = jnp.sum(total, axis=0, keepdims=True)

    for t, spot in enumerate(spots):
        go(remote(l0, b1.at[t], ls.at[t], lr.at[t], near(*spot)))
    for t in (1, 2, 3):
        peer = at_x(me, t)
        go(remote(made.at[peer[1]], grad.at[group], gs.at[t], gr.at[t], peer))
    keep = pltpu.make_async_copy(made.at[x], grad.at[group], gs.at[0])
    keep.start()
    for t, (dx, dc, dy) in enumerate(spots):
        remote(b1.at[t], b1.at[t], ls.at[t], lr.at[t], near(-dx, dc, -dy)).wait_recv()
    l1[...] = l0[...] + jnp.sum(b1[...], axis=0)
    for t in range(7):
        go(remote(l1, b2.at[t], zs2.at[t], zr2.at[t], at_z(me, t + 1)))
    for t in range(7):
        remote(b2.at[t], b2.at[t], zs2.at[t], zr2.at[t], at_z(me, -t - 1)).wait_recv()
    value = l1[...] + jnp.sum(b2[...], axis=0)
    loss[...] = jnp.sum(value, axis=1, keepdims=True) * (1.0 / 6553600.0)
    keep.wait()
    for t in (1, 2, 3):
        peer = at_x(me, -t)
        there = pl.ds(pl.multiple_of(32 * peer[1], 32), 32)
        remote(grad.at[there], grad.at[there], gs.at[t], gr.at[t], peer).wait_recv()
    for copy in started:
        copy.wait_send()
    for m in range(4):
        for t in (1, 2, 3):
            to_x(m, t).wait_send()
        to_other(m).wait_send()


def dma(*shape):
    return pltpu.SemaphoreType.DMA(shape)


def per_device(
    node_states, noise, norm_gain, cond_weight, w_query, w_key, w_value, w_out,
    edge_src, send_rows, dec_src, dec_weight, w_decode, truth, area,
):
    grad, loss = pl.pallas_call(
        step_kernel,
        out_shape=(
            jax.ShapeDtypeStruct((128, 1024), BF16),
            jax.ShapeDtypeStruct((1, 1), F32),
        ),
        in_specs=[pl.BlockSpec(memory_space=pl.ANY)] * 15,
        out_specs=(pl.BlockSpec(memory_space=pl.ANY), VMEM),
        scratch_shapes=[
            pltpu.VMEM((256, 1024), BF16),
            pltpu.VMEM((16, 256), BF16),
            pltpu.VMEM((1, 256), jnp.int32),
            pltpu.VMEM((1, 1024), F32),
            pltpu.VMEM((16, 2048), BF16),
            pltpu.VMEM((8, 256), jnp.int32),
            pltpu.VMEM((100, 1024), BF16),
            pltpu.VMEM((3, 1024), jnp.int32),
            pltpu.VMEM((3, 1024), F32),
            pltpu.VMEM((100, 1024), BF16),
            pltpu.VMEM((1, 1024), F32),
            pltpu.VMEM((16, 1024), BF16),
            pltpu.VMEM((8, 4, 2, 16, 896), BF16),
            pltpu.VMEM((2, 128, 1024), BF16),
            pltpu.VMEM((4, 2, 16, 128), BF16),
            pltpu.VMEM((4, 16, 256), BF16),
            pltpu.VMEM((2, 128, 1024), BF16),
            pltpu.VMEM((2, 16, 128), BF16),
            pltpu.VMEM((512, 1024), F32),
            pltpu.VMEM((256, 512), F32),
            pltpu.VMEM((4, 512, 1024), BF16),
            pltpu.VMEM((16, 128), BF16),
            pltpu.VMEM((128, 256), BF16),
            pltpu.VMEM((256, 256), F32),
            pltpu.VMEM((4, 128, 256), BF16),
            pltpu.VMEM((4, 4, 32, 256), BF16),
            pltpu.VMEM((4, 32, 256), BF16),
            pltpu.VMEM((4, 32, 256), BF16),
            pltpu.VMEM((2, 256, 1024), BF16),
            pltpu.VMEM((128, 1024), F32),
            pltpu.VMEM((8, 32, 1024), F32),
            pltpu.VMEM((4, 32, 1024), F32),
            pltpu.VMEM((128, 1024), F32),
            pltpu.VMEM((4, 32, 1024), BF16),
            pltpu.VMEM((1, 128), F32),
            pltpu.VMEM((1, 128), F32),
            pltpu.VMEM((31, 1, 128), F32),
            pltpu.VMEM((7, 1, 128), F32),
            dma(16),
            dma(8), dma(8), dma(8, 3), dma(8, 3), dma(8), dma(8), dma(2), dma(2), dma(2), dma(2),
            dma(4, 3), dma(4, 3), dma(4, 4), dma(4, 4), dma(4), dma(4), dma(4), dma(4),
            dma(31), dma(31), dma(7), dma(7),
        ],
        compiler_params=pltpu.CompilerParams(collective_id=0, has_side_effects=True),
        name="step",
    )(
        w_query, w_key, w_value, w_out, node_states, noise[0], send_rows.reshape(1, 256),
        norm_gain.reshape(1, 1024), cond_weight, edge_src, w_decode,
        dec_src, dec_weight, truth, area.reshape(1, 1024),
    )
    return loss[0, 0], grad[None, :100]


def solution(mesh):
    split = Mesh(mesh.devices.reshape(2, 4, 8, 4, 2), MEMBER + SPACE)
    return jax.shard_map(
        per_device,
        mesh=split,
        in_specs=(
            P(SPACE, None),
            P(MEMBER, None, SPACE),
            P(),
            P(),
            P(SPACE, None),
            P(SPACE, None),
            P(SPACE, None),
            P(SPACE, None),
            P(None, SPACE),
            P(SPACE),
            P(None, SPACE),
            P(None, SPACE),
            P(),
            P(None, SPACE),
            P(SPACE),
        ),
        out_specs=(P(), P(MEMBER, None, SPACE)),
        check_vma=False,
    )
```
